128 devices in a mesh: shard: 16 (over z_hi, x, core), tp: 8 (over z_lo, y).
Axes of the slice: x: 4, y: 4, z: 4 (z_hi: 2, z_lo: 2; z = z_hi * 2 + z_lo), core: 2. Of those that a mesh axis runs over, the one named last changes fastest.
Arguments:
- train_query: bfloat16 [5120, 8192], P('shard', 'tp'), may hold values from -0.078125 to 0.078125
- low_query: bfloat16 [5120, 32], P('shard'), may hold values from -0.078125 to 0.078125
- high_query: bfloat16 [32, 8192], P(None, 'tp'), may hold values from -1 to 1
- train_key: bfloat16 [5120, 1024], P('shard', 'tp'), may hold values from -0.078125 to 0.078125
- low_key: bfloat16 [5120, 32], P('shard'), may hold values from -0.078125 to 0.078125
- high_key: bfloat16 [32, 1024], P(None, 'tp'), may hold values from -1 to 1
- train_value: bfloat16 [5120, 1024], P('shard', 'tp'), may hold values from -0.078125 to 0.078125
- low_value: bfloat16 [5120, 32], P('shard'), may hold values from -0.078125 to 0.078125
- high_value: bfloat16 [32, 1024], P(None, 'tp'), may hold values from -1 to 1
- train_mixed: bfloat16 [8192, 5120], P('tp', 'shard'), may hold values from -0.0625 to 0.0625
- low_mixed: bfloat16 [8192, 32], P('tp'), may hold values from -0.0625 to 0.0625
- high_mixed: bfloat16 [32, 5120], P(None, 'shard'), may hold values from -1 to 1
- norm_train: float32 [5120], P(('shard', 'tp')), may hold values from 0.25 to 1.75
- norm_step: float32 [5120], P(('shard', 'tp')), may hold values from -0.3 to 0.3
Outputs:
- final_query: bfloat16 [5120, 8192], P(None, 'tp')
- final_key: bfloat16 [5120, 1024], P(None, 'tp')
- final_value: bfloat16 [5120, 1024], P(None, 'tp')
- final_mixed: bfloat16 [8192, 5120], P('tp')
- serve_norm: bfloat16 [5120], replicated
The draws below stay inside these ranges and needn't reach their ends.
All inputs are finite; a program needn't handle non-finite values.
Results may differ from the reference program's by a relative error of at most 0.001.
Values may be sent and summed in bfloat16 or wider, within the bound.
A program may use at most 128 MiB of HBM per device.

```python
import jax
import jax.numpy as jnp

D_MODEL = 5120
Q_DIM = 8192
KV_DIM = 1024
RANK = 32


def block_scale(rng, shape, shards, low, top_value):
    gain = 1.0
    for position, parts in shards:
        steps = jax.random.uniform(jax.random.fold_in(jax.random.fold_in(rng, 6), position), (parts,), jnp.float32, low / len(shards), top_value / len(shards))
        gain = gain * jnp.repeat(jnp.exp(steps), shape[position] // parts).reshape((-1,) + (1,) * (len(shape) - 1 - position))
    return gain


def noise(rng, extent, width, bound, split=(), held_as=jnp.bfloat16):
    values = width * jax.random.normal(rng, extent, jnp.float32)
    if split:
        values = values * block_scale(rng, extent, split, -0.22, 0.18)
    return jnp.clip(values, -bound, bound).astype(held_as)


def setup_inputs(seed: int = 0) -> dict:
    key_list = jax.random.split(jax.random.key(seed), 15)
    return {
        "train_query": noise(key_list[0], (D_MODEL, Q_DIM), D_MODEL ** -0.5, 0.078125, ((0, 16), (1, 8))),
        "low_query": noise(key_list[1], (D_MODEL, RANK), D_MODEL ** -0.5, 0.078125, ((0, 16),)),
        "high_query": noise(key_list[2], (RANK, Q_DIM), RANK ** -0.5, 1.0, ((1, 8),)),
        "train_key": noise(key_list[3], (D_MODEL, KV_DIM), D_MODEL ** -0.5, 0.078125, ((0, 16), (1, 8))),
        "low_key": noise(key_list[4], (D_MODEL, RANK), D_MODEL ** -0.5, 0.078125, ((0, 16),)),
        "high_key": noise(key_list[5], (RANK, KV_DIM), RANK ** -0.5, 1.0, ((1, 8),)),
        "train_value": noise(key_list[6], (D_MODEL, KV_DIM), D_MODEL ** -0.5, 0.078125, ((0, 16), (1, 8))),
        "low_value": noise(key_list[7], (D_MODEL, RANK), D_MODEL ** -0.5, 0.078125, ((0, 16),)),
        "high_value": noise(key_list[8], (RANK, KV_DIM), RANK ** -0.5, 1.0, ((1, 8),)),
        "train_mixed": noise(key_list[9], (Q_DIM, D_MODEL), Q_DIM ** -0.5, 0.0625, ((0, 8), (1, 16))),
        "low_mixed": noise(key_list[10], (Q_DIM, RANK), Q_DIM ** -0.5, 0.0625, ((0, 8),)),
        "high_mixed": noise(key_list[11], (RANK, D_MODEL), RANK ** -0.5, 1.0, ((1, 16),)),
        "norm_train": jnp.clip(1.0 + 0.15 * jax.random.normal(key_list[12], (D_MODEL,), jnp.float32), 0.25, 1.75),
        "norm_step": jnp.clip(jax.random.uniform(key_list[13], (D_MODEL,), jnp.float32, -0.3, 0.3) * block_scale(key_list[13], (D_MODEL,), ((0, 128),), -0.4, 0.0), -0.3, 0.3),
    }


mix_rate = 0.5


def reference(train_query, low_query, high_query, train_key, low_key, high_key, train_value, low_value, high_value, train_mixed, low_mixed, high_mixed, norm_train, norm_step):
    result_query = train_query.astype(jnp.float32) + mix_rate * jnp.dot(low_query, high_query, preferred_element_type=jnp.float32)
    result_key = train_key.astype(jnp.float32) + mix_rate * jnp.dot(low_key, high_key, preferred_element_type=jnp.float32)
    result_value = train_value.astype(jnp.float32) + mix_rate * jnp.dot(low_value, high_value, preferred_element_type=jnp.float32)
    result_mixed = train_mixed.astype(jnp.float32) + mix_rate * jnp.dot(low_mixed, high_mixed, preferred_element_type=jnp.float32)
    final_query = result_query.astype(jnp.bfloat16)
    final_key = result_key.astype(jnp.bfloat16)
    final_value = result_value.astype(jnp.bfloat16)
    final_mixed = result_mixed.astype(jnp.bfloat16)
    serve_norm = (norm_train + norm_step).astype(jnp.bfloat16)
    return final_query, final_key, final_value, final_mixed, serve_norm
```

```python
import functools
import heapq

import jax
import jax.numpy as jnp
from jax import lax
from jax.experimental import pallas as pl
from jax.experimental.pallas import tpu as pltpu
from jax.sharding import PartitionSpec as P

MESH = pl.DeviceIdType.MESH
mix_rate = 0.5

Q_ROWS = 80
M_ROWS = 128
HALF = (0, 0, 0, 1, 1, 1, 0, 0, 1, 1)
IS_B = (0,) * 6 + (1,) * 4
SIZES = (163840, 163840, 81920, 163840, 163840, 81920) + (163840,) * 4
N_CHUNKS = 10
RELAY_SLOT = {0: 0, 1: 1, 2: 2, 3: 0, 4: 1, 5: 2}


def own_sends(chunk, along_x, along_z):
    sends = []
    if along_z:
        sends.append(("z+", ("r+", 0, chunk)) if HALF[chunk] == 0 else ("z-", ("r-", 0, chunk)))
    if along_x:
        sends += [("x+", ("x+", 0, 3, chunk)), ("x-", ("x-", 0, 1, chunk))]
    if along_z:
        sends.append(("d", ("d", 0, 0, chunk)))
    return sends


def react(event):
    kind = event[0]
    if kind in ("r+", "r-"):
        return [("z" + kind[1], ("z",) + event[1:])]
    if kind == "z":
        _, dx, chunk = event
        sends = [("d", ("d", 1, dx, chunk))]
        if not IS_B[chunk]:
            sends += [("x+", ("x+", 1, 3, chunk)), ("x-", ("x-", 1, 1, chunk))]
        return sends
    _, dz, dx, chunk = event
    sends = []
    if kind == "x+" and dx == 3 and HALF[chunk] == 0:
        sends.append(("x+", ("x+", dz, 2, chunk)))
    if kind == "x-" and dx == 1 and HALF[chunk] == 1:
        sends.append(("x-", ("x-", dz, 2, chunk)))
    if IS_B[chunk] and dz == 0:
        sends.append(("z+", ("r+", dx, chunk)) if HALF[chunk] == 0 else ("z-", ("r-", dx, chunk)))
    sends.append(("d", ("d", dz, dx, chunk)))
    return sends


def plan():
    first = []
    for chunk in (0, 3):
        first += own_sends(chunk, True, True)
    second = []
    for chunk in (1, 4, 2, 5):
        second += own_sends(chunk, False, True)
    third = []
    for chunk in (6, 8, 7, 9):
        third += own_sends(chunk, True, True)
    for chunk in (1, 4, 2, 5):
        third += own_sends(chunk, True, False)
    starts = [(3.5, first), (4.0, second), (8.0, third)]
    heap, count, free, order = [], 0, {}, []
    for time, sends in starts:
        heapq.heappush(heap, (time, count, None, sends))
        count += 1
    while heap:
        time, _, event, sends = heapq.heappop(heap)
        if event is not None:
            order.append((time, event))
            sends = react(event)
        for link, item in sends:
            if link == "d":
                continue
            done = max(time, free.get(link, 0.0)) + SIZES[item[-1]] / 45000.0
            free[link] = done
            heapq.heappush(heap, (done + 1.9, count, item, None))
            count += 1
    order += [(9.0, ("ny",)), (32.0, ("nz",)), (56.0, ("nx",))]
    order = [event for _, event in sorted(order, key=lambda pair: pair[0])]
    return first, second, third, order


def count_sends():
    first, second, third, order = plan()
    total = len(first) + len(second) + len(third)
    for event in order:
        if event[0][0] != "n":
            total += len(react(event))
    return total + 2 + 3 + 3 + 3 + 4


N_SENDS = count_sends()
N_LOADS = 14


def gather_kernel(
    tq, lq, hq, tk, lk, hk, tv, lv, hv, tm, lm, hm, n1, n2,
    q_all, k_all, v_all, m_all, n_all,
    tq_v, lq_v, hq_v, tk_v, lk_v, hk_v, tv_v, lv_v, hv_v, tm_v, lm_v, hm_v, n1_v, n2_v,
    tm_s, hm_s, turn, relay_q, relay_kv, relay_m,
    load_sem, send_sem, arrive_sem, relay_sem, sib_sem, pair_sem, norm_sem,
):
    sh = lax.axis_index("shard")
    tp = lax.axis_index("tp")
    core = lax.rem(sh, 2)
    x = lax.rem(sh // 2, 4)
    z = (sh // 8) * 2 + tp // 4
    y = lax.rem(tp, 4)

    def device(dx=0, dz=0, dy=0, other=False):
        zz = lax.rem(z + dz, 4)
        cc = 1 - core if other else core
        return (
            ((zz // 2) * 4 + lax.rem(x + dx, 4)) * 2 + cc,
            lax.rem(zz, 2) * 4 + lax.rem(y + dy, 4),
        )

    target = {
        "x+": device(dx=1), "x-": device(dx=3), "z+": device(dz=1), "z-": device(dz=3), "d": device(other=True),
    }

    loads = []
    for k, (src, dst) in enumerate((
        (tq, tq_v), (lq, lq_v), (hq, hq_v), (tm, tm_v), (hm, hm_v), (lm, lm_v), (tk, tk_v), (lk, lk_v), (hk, hk_v),
        (tv, tv_v), (lv, lv_v), (hv, hv_v), (n1, n1_v), (n2, n2_v),
    )):
        copy = pltpu.make_async_copy(src, dst, load_sem.at[k])
        copy.start()
        loads.append(copy)

    partners = [device(dx=k) for k in (1, 2, 3)] + [device(dz=k) for k in (1, 2, 3)]
    partners += [device(dy=k) for k in (1, 2, 3)] + [device(other=True)]
    barrier = pltpu.get_barrier_semaphore()
    for partner in partners:
        pl.semaphore_signal(barrier, inc=1, device_id=partner, device_id_type=MESH)
    pl.semaphore_wait(barrier, len(partners))

    started = []

    def send(src, dst, sem, to):
        copy = pltpu.make_async_remote_copy(
            src_ref=src, dst_ref=dst, send_sem=send_sem.at[len(started)], recv_sem=sem,
            device_id=to, device_id_type=MESH,
        )
        copy.start()
        started.append(copy)

    def arrived(dst, sem):
        pltpu.make_async_remote_copy(
            src_ref=dst, dst_ref=dst, send_sem=send_sem.at[0], recv_sem=sem,
            device_id=target["d"], device_id_type=MESH,
        ).wait_recv()

    def place(chip, cc, chunk):
        row = (chip * 2 + cc) * 320
        if chunk in (2, 5):
            return (k_all if chunk == 2 else v_all).at[pl.ds(pl.multiple_of(row, 64), 320)]
        if chunk < 6:
            part = chunk if chunk < 2 else chunk - 1
            return q_all.at[pl.ds(pl.multiple_of(row + Q_ROWS * part, 16), Q_ROWS)]
        return m_all.at[chip, pl.ds(pl.multiple_of(512 * cc + M_ROWS * (chunk - 6), M_ROWS), M_ROWS)]

    def chip_at(dz2, dx):
        return (lax.rem(sh // 8 + dz2, 2)) * 4 + lax.rem(x + dx, 4)

    def relay_place(way, dx, chunk):
        if chunk in (2, 5):
            return relay_kv.at[way]
        if chunk < 6:
            return relay_q.at[way, pl.ds(Q_ROWS * (chunk % 3), Q_ROWS)]
        return relay_m.at[way, dx, pl.ds(M_ROWS * (chunk % 2), M_ROWS)]

    def relay_index(way, dx, chunk):
        return way * 11 + (chunk % 3 if chunk < 6 else 3 + dx * 2 + chunk % 2)

    def arrive_index(dz, dx, chunk):
        return (dz * 4 + dx) * N_CHUNKS + chunk

    def dispatch(link, item, src, chip):
        kind, chunk = item[0], item[-1]
        if kind in ("r+", "r-"):
            way = HALF[chunk]
            dst, sem = relay_place(way, item[1], chunk), relay_sem.at[relay_index(way, item[1], chunk)]
        elif kind == "d":
            dst, sem = src, sib_sem.at[arrive_index(item[1], item[2], chunk)]
        elif kind == "z":
            dst, sem = place(chip, core, chunk), arrive_sem.at[arrive_index(1, item[1], chunk)]
        else:
            dst, sem = src, arrive_sem.at[arrive_index(item[1], item[2], chunk)]
        send(src, dst, sem, target[link])

    first, second, third, order = plan()
    own = chip_at(0, 0)

    def wait_loads(*which):
        for k in which:
            loads[k].wait()

    half = pl.ds(pl.multiple_of(512 * core, 512), 512)
    other_half = pl.ds(pl.multiple_of(512 * (1 - core), 512), 512)
    wait_loads(3, 4)
    send(tm_v.at[:, other_half], tm_s, pair_sem.at[0], target["d"])
    send(hm_v, hm_s, pair_sem.at[1], target["d"])

    def product(low_turned, high):
        return mix_rate * lax.dot_general(
            low_turned, high, (((0,), (0,)), ((), ())), preferred_element_type=jnp.float32
        )

    row = sh * 320
    wait_loads(0, 1, 2)
    q_all[pl.ds(pl.multiple_of(row, 64), 320)] = (
        tq_v[...].astype(jnp.float32) + product(lq_v[...], hq_v[...])
    ).astype(jnp.bfloat16)
    wait_loads(12, 13)
    n_at = (x * 2 + core) * 4 + z
    n_all[n_at, y] = jnp.zeros((1, 128), jnp.float32)
    n_all[n_at, y, :, 0:40] = n1_v[...] + n2_v[...]
    for link, item in first:
        dispatch(link, item, place(own, core, item[-1]), own)
    wait_loads(6, 7, 8, 9, 10, 11)
    k_all[pl.ds(pl.multiple_of(row, 64), 320)] = (
        tk_v[...].astype(jnp.float32) + product(lk_v[...], hk_v[...])
    ).astype(jnp.bfloat16)
    v_all[pl.ds(pl.multiple_of(row, 64), 320)] = (
        tv_v[...].astype(jnp.float32) + product(lv_v[...], hv_v[...])
    ).astype(jnp.bfloat16)
    for k in (1, 2, 3):
        send(n_all.at[n_at, y], n_all.at[n_at, y], norm_sem.at[k - 1], device(dy=k))
    for link, item in second:
        dispatch(link, item, place(own, core, item[-1]), own)

    wait_loads(5)
    arrived(tm_s, pair_sem.at[0])
    arrived(hm_s, pair_sem.at[1])
    mine = pl.ds(pl.multiple_of(320 * core, 64), 320)
    others = pl.ds(pl.multiple_of(320 * (1 - core), 64), 320)
    low_half = lm_v[:, half]
    own_half = tm_v[:, half]
    for b in range(4):
        cols = slice(M_ROWS * b, M_ROWS * (b + 1))
        low = low_half[:, cols]
        turn[b, mine] = own_half[:, cols].astype(jnp.float32) + product(hm_v[...], low)
        turn[b, others] = tm_s[:, cols].astype(jnp.float32) + product(hm_s[...], low)
        rows = pl.ds(pl.multiple_of(512 * core + M_ROWS * b, M_ROWS), M_ROWS)
        m_all[own, rows] = turn[b].T.astype(jnp.bfloat16)
    for link, item in third:
        dispatch(link, item, place(own, core, item[-1]), own)

    for event in order:
        kind, chunk = event[0], event[-1]
        if kind == "ny":
            for k in (1, 2, 3):
                arrived(n_all.at[n_at, lax.rem(y + 4 - k, 4)], norm_sem.at[k - 1])
            for k in (1, 2, 3):
                send(n_all.at[n_at], n_all.at[n_at], norm_sem.at[3 + k - 1], device(dz=k))
        elif kind == "nz":
            block = (x * 2 + core) * 4
            for k in (1, 2, 3):
                arrived(n_all.at[block + lax.rem(z + 4 - k, 4)], norm_sem.at[3 + k - 1])
            line = n_all.at[pl.ds(block, 4)]
            for k in (1, 2, 3):
                send(line, line, norm_sem.at[6 + k - 1], device(dx=k))
            send(line, line, norm_sem.at[9], target["d"])
        elif kind == "nx":
            for k in (1, 2, 3):
                line = n_all.at[pl.ds((lax.rem(x + 4 - k, 4) * 2 + core) * 4, 4)]
                arrived(line, norm_sem.at[6 + k - 1])
                send(line, line, norm_sem.at[9 + k], target["d"])
        elif kind in ("r+", "r-"):
            way = HALF[chunk]
            src = relay_place(way, event[1], chunk)
            arrived(src, relay_sem.at[relay_index(way, event[1], chunk)])
            from_z = lax.rem(z + (3 if way == 0 else 1), 4)
            chip = (from_z // 2) * 4 + lax.rem(x + event[1], 4)
            for link, item in react(event):
                dispatch(link, item, src, chip)
        else:
            dz, dx = (1, event[1]) if kind == "z" else (event[1], event[2])
            chip = chip_at(dz, dx)
            src = place(chip, core, chunk)
            arrived(src, arrive_sem.at[arrive_index(dz, dx, chunk)])
            for link, item in react(event):
                dispatch(link, item, src, chip)

    for dz in (0, 1):
        for dx in range(4):
            for chunk in range(N_CHUNKS):
                arrived(place(chip_at(dz, dx), 1 - core, chunk), sib_sem.at[arrive_index(dz, dx, chunk)])
    for k in range(4):
        line = n_all.at[pl.ds((lax.rem(x + 4 - k, 4) * 2 + 1 - core) * 4, 4)]
        arrived(line, norm_sem.at[9 + k])
    for copy in started:
        copy.wait_send()


def write_kernel(q_all, k_all, v_all, m_all, n_all, q_out, k_out, v_out, m_out, n_out, lines, sems):
    copies = []
    for k in range(8):
        copies.append((m_all.at[k], m_out.at[:, pl.ds(640 * k, 640)]))
        copies.append((q_all.at[pl.ds(640 * k, 640)], q_out.at[pl.ds(640 * k, 640)]))
    copies += [(k_all, k_out), (v_all, v_out)]
    copies = [pltpu.make_async_copy(src, dst, sems.at[k]) for k, (src, dst) in enumerate(copies)]
    for copy in copies:
        copy.start()
    lane = lax.broadcasted_iota(jnp.int32, (8, 128), 1)
    acc = [jnp.zeros((8, 128), jnp.float32) for _ in range(5)]
    for i in range(16):
        core, zl, y = i // 8, (i // 4) % 2, i % 4
        rows = [n_all[(xx * 2 + core) * 4 + zh * 2 + zl, y] for zh in range(2) for xx in range(4)]
        block = jnp.concatenate(rows, axis=0)
        q, off = (40 * i) // 128, (40 * i) % 128
        turned = pltpu.roll(block, off, 1) if off else block
        acc[q] = jnp.where((lane >= off) & (lane < off + 40), turned, acc[q])
        if off + 40 > 128:
            acc[q + 1] = jnp.where(lane < off + 40 - 128, turned, acc[q + 1])
    for q in range(5):
        lines[pl.ds(q, 8, stride=5), :] = acc[q]
    n_out[...] = lines[...].astype(jnp.bfloat16)
    for copy in copies:
        copy.wait()


def body(
    train_query, low_query, high_query, train_key, low_key, high_key, train_value, low_value, high_value,
    train_mixed, low_mixed, high_mixed, norm_train, norm_step,
):
    bf16, f32 = jnp.bfloat16, jnp.float32
    args = (
        train_query, low_query.T, high_query, train_key, low_key.T, high_key, train_value, low_value.T, high_value,
        train_mixed.T, low_mixed.T, high_mixed, norm_train.reshape(1, -1), norm_step.reshape(1, -1),
    )
    vmem = pltpu.MemorySpace.VMEM
    q_all, k_all, v_all, m_all, n_all = pl.pallas_call(
        gather_kernel,
        name="gather",
        out_shape=[
            vmem((5120, 1024), bf16), vmem((5120, 128), bf16), vmem((5120, 128), bf16),
            vmem((8, 1024, 640), bf16), vmem((32, 4, 1, 128), f32),
        ],
        in_specs=[pl.BlockSpec(memory_space=pltpu.MemorySpace.HBM)] * 14,
        out_specs=[pl.BlockSpec(memory_space=vmem)] * 5,
        scratch_shapes=[pltpu.VMEM(a.shape, a.dtype) for a in args] + [
            pltpu.VMEM((320, 512), bf16), pltpu.VMEM((32, 320), bf16), pltpu.VMEM((4, 640, 128), f32),
            pltpu.VMEM((2, 160, 1024), bf16), pltpu.VMEM((2, 320, 128), bf16), pltpu.VMEM((2, 4, 256, 640), bf16),
            pltpu.SemaphoreType.DMA((N_LOADS,)), pltpu.SemaphoreType.DMA((N_SENDS,)),
            pltpu.SemaphoreType.DMA((80,)), pltpu.SemaphoreType.DMA((22,)), pltpu.SemaphoreType.DMA((80,)),
            pltpu.SemaphoreType.DMA((2,)), pltpu.SemaphoreType.DMA((13,)),
        ],
        compiler_params=pltpu.CompilerParams(
            collective_id=0, has_side_effects=True, vmem_limit_bytes=36 * 1024 * 1024
        ),
    )(*args)
    hbm = pltpu.MemorySpace.HBM
    q, k, v, m, n = pl.pallas_call(
        write_kernel,
        name="write",
        out_shape=[
            jax.ShapeDtypeStruct((5120, 1024), bf16), jax.ShapeDtypeStruct((5120, 128), bf16),
            jax.ShapeDtypeStruct((5120, 128), bf16), jax.ShapeDtypeStruct((1024, 5120), bf16),
            jax.ShapeDtypeStruct((40, 128), bf16),
        ],
        in_specs=[pl.BlockSpec(memory_space=vmem)] * 5,
        out_specs=[pl.BlockSpec(memory_space=hbm)] * 4 + [pl.BlockSpec(memory_space=vmem)],
        scratch_shapes=[pltpu.VMEM((40, 128), f32), pltpu.SemaphoreType.DMA((18,))],
        compiler_params=pltpu.CompilerParams(vmem_limit_bytes=36 * 1024 * 1024),
    )(q_all, k_all, v_all, m_all, n_all)
    return q, k, v, m, n.reshape(5120)


def solution(mesh):
    return jax.shard_map(
        body,
        mesh=mesh,
        in_specs=(
            P("shard", "tp"), P("shard", None), P(None, "tp"),
            P("shard", "tp"), P("shard", None), P(None, "tp"),
            P("shard", "tp"), P("shard", None), P(None, "tp"),
            P("tp", "shard"), P("tp", None), P(None, "shard"),
            P(("shard", "tp")), P(("shard", "tp")),
        ),
        out_specs=(P(None, "tp"), P(None, "tp"), P(None, "tp"), P("tp", None), P()),
        check_vma=False,
    )
```

```python
import functools
import heapq

import jax
import jax.numpy as jnp
from jax import lax
from jax.experimental import pallas as pl
from jax.experimental.pallas import tpu as pltpu
from jax.sharding import PartitionSpec as P

MESH = pl.DeviceIdType.MESH
mix_rate = 0.5

Q_ROWS = 80
M_ROWS = 128
HALF = (0, 0, 0, 1, 1, 1, 0, 0, 1, 1)
IS_B = (0,) * 6 + (1,) * 4
SIZES = (163840, 163840, 81920, 163840, 163840, 81920) + (163840,) * 4
N_CHUNKS = 10
RELAY_SLOT = {0: 0, 1: 1, 2: 2, 3: 0, 4: 1, 5: 2}


def own_sends(chunk, along_x, along_z):
    sends = []
    if along_z:
        sends.append(("z+", ("r+", 0, chunk)) if HALF[chunk] == 0 else ("z-", ("r-", 0, chunk)))
    if along_x:
        sends += [("x+", ("x+", 0, 3, chunk)), ("x-", ("x-", 0, 1, chunk))]
    if along_z:
        sends.append(("d", ("d", 0, 0, chunk)))
    return sends


def react(event):
    kind = event[0]
    if kind in ("r+", "r-"):
        return [("z" + kind[1], ("z",) + event[1:])]
    if kind == "z":
        _, dx, chunk = event
        sends = [("d", ("d", 1, dx, chunk))]
        if not IS_B[chunk]:
            sends += [("x+", ("x+", 1, 3, chunk)), ("x-", ("x-", 1, 1, chunk))]
        return sends
    _, dz, dx, chunk = event
    sends = []
    if kind == "x+" and dx == 3 and HALF[chunk] == 0:
        sends.append(("x+", ("x+", dz, 2, chunk)))
    if kind == "x-" and dx == 1 and HALF[chunk] == 1:
        sends.append(("x-", ("x-", dz, 2, chunk)))
    if IS_B[chunk] and dz == 0:
        sends.append(("z+", ("r+", dx, chunk)) if HALF[chunk] == 0 else ("z-", ("r-", dx, chunk)))
    sends.append(("d", ("d", dz, dx, chunk)))
    return sends


def plan():
    first = []
    for chunk in (0, 3):
        first += own_sends(chunk, True, True)
    second = []
    for chunk in (1, 4, 2, 5):
        second += own_sends(chunk, False, True)
    third = []
    for chunk in (6, 8, 7, 9):
        third += own_sends(chunk, True, True)
    for chunk in (1, 4, 2, 5):
        third += own_sends(chunk, True, False)
    starts = [(3.5, first), (4.0, second), (8.0, third)]
    heap, count, free, order = [], 0, {}, []
    for time, sends in starts:
        heapq.heappush(heap, (time, count, None, sends))
        count += 1
    while heap:
        time, _, event, sends = heapq.heappop(heap)
        if event is not None:
            order.append((time, event))
            sends = react(event)
        for link, item in sends:
            if link == "d":
                continue
            done = max(time, free.get(link, 0.0)) + SIZES[item[-1]] / 45000.0
            free[link] = done
            heapq.heappush(heap, (done + 1.9, count, item, None))
            count += 1
    order += [(9.0, ("ny",)), (32.0, ("nz",)), (56.0, ("nx",))]
    order = [event for _, event in sorted(order, key=lambda pair: pair[0])]
    return first, second, third, order


def count_sends():
    first, second, third, order = plan()
    total = len(first) + len(second) + len(third)
    for event in order:
        if event[0][0] != "n":
            total += len(react(event))
    return total + 2 + 3 + 3 + 3 + 4


N_SENDS = count_sends()
N_LOADS = 14


def gather_kernel(
    tq, lq, hq, tk, lk, hk, tv, lv, hv, tm, lm, hm, n1, n2,
    q_all, k_all, v_all, m_all, n_all,
    tq_v, lq_v, hq_v, tk_v, lk_v, hk_v, tv_v, lv_v, hv_v, tm_v, lm_v, hm_v, n1_v, n2_v,
    tm_s, hm_s, turn, relay_q, relay_kv, relay_m,
    load_sem, send_sem, arrive_sem, relay_sem, sib_sem, pair_sem, norm_sem,
):
    sh = lax.axis_index("shard")
    tp = lax.axis_index("tp")
    core = lax.rem(sh, 2)
    x = lax.rem(sh // 2, 4)
    z = (sh // 8) * 2 + tp // 4
    y = lax.rem(tp, 4)

    def device(dx=0, dz=0, dy=0, other=False):
        zz = lax.rem(z + dz, 4)
        cc = 1 - core if other else core
        return (
            ((zz // 2) * 4 + lax.rem(x + dx, 4)) * 2 + cc,
            lax.rem(zz, 2) * 4 + lax.rem(y + dy, 4),
        )

    target = {
        "x+": device(dx=1), "x-": device(dx=3), "z+": device(dz=1), "z-": device(dz=3), "d": device(other=True),
    }

    loads = []
    for k, (src, dst) in enumerate((
        (tq, tq_v), (lq, lq_v), (hq, hq_v), (tm, tm_v), (hm, hm_v), (lm, lm_v), (tk, tk_v), (lk, lk_v), (hk, hk_v),
        (tv, tv_v), (lv, lv_v), (hv, hv_v), (n1, n1_v), (n2, n2_v),
    )):
        copy = pltpu.make_async_copy(src, dst, load_sem.at[k])
        copy.start()
        loads.append(copy)

    partners = [device(dx=k) for k in (1, 2, 3)] + [device(dz=k) for k in (1, 2, 3)]
    partners += [device(dy=k) for k in (1, 2, 3)] + [device(other=True)]
    barrier = pltpu.get_barrier_semaphore()
    for partner in partners:
        pl.semaphore_signal(barrier, inc=1, device_id=partner, device_id_type=MESH)
    pl.semaphore_wait(barrier, len(partners))

    started = []

    def send(src, dst, sem, to):
        copy = pltpu.make_async_remote_copy(
            src_ref=src, dst_ref=dst, send_sem=send_sem.at[len(started)], recv_sem=sem,
            device_id=to, device_id_type=MESH,
        )
        copy.start()
        started.append(copy)

    def arrived(dst, sem):
        pltpu.make_async_remote_copy(
            src_ref=dst, dst_ref=dst, send_sem=send_sem.at[0], recv_sem=sem,
            device_id=target["d"], device_id_type=MESH,
        ).wait_recv()

    def place(chip, cc, chunk):
        row = (chip * 2 + cc) * 320
        if chunk in (2, 5):
            return (k_all if chunk == 2 else v_all).at[pl.ds(pl.multiple_of(row, 64), 320)]
        if chunk < 6:
            part = chunk if chunk < 2 else chunk - 1
            return q_all.at[pl.ds(pl.multiple_of(row + Q_ROWS * part, 16), Q_ROWS)]
        return m_all.at[chip, pl.ds(pl.multiple_of(512 * cc + M_ROWS * (chunk - 6), M_ROWS), M_ROWS)]

    def chip_at(dz2, dx):
        return (lax.rem(sh // 8 + dz2, 2)) * 4 + lax.rem(x + dx, 4)

    def relay_place(way, dx, chunk):
        if chunk in (2, 5):
            return relay_kv.at[way]
        if chunk < 6:
            return relay_q.at[way, pl.ds(Q_ROWS * (chunk % 3), Q_ROWS)]
        return relay_m.at[way, dx, pl.ds(M_ROWS * (chunk % 2), M_ROWS)]

    def relay_index(way, dx, chunk):
        return way * 11 + (chunk % 3 if chunk < 6 else 3 + dx * 2 + chunk % 2)

    def arrive_index(dz, dx, chunk):
        return (dz * 4 + dx) * N_CHUNKS + chunk

    def dispatch(link, item, src, chip):
        kind, chunk = item[0], item[-1]
        if kind in ("r+", "r-"):
            way = HALF[chunk]
            dst, sem = relay_place(way, item[1], chunk), relay_sem.at[relay_index(way, item[1], chunk)]
        elif kind == "d":
            dst, sem = src, sib_sem.at[arrive_index(item[1], item[2], chunk)]
        elif kind == "z":
            dst, sem = place(chip, core, chunk), arrive_sem.at[arrive_index(1, item[1], chunk)]
        else:
            dst, sem = src, arrive_sem.at[arrive_index(item[1], item[2], chunk)]
        send(src, dst, sem, target[link])

    first, second, third, order = plan()
    own = chip_at(0, 0)

    def wait_loads(*which):
        for k in which:
            loads[k].wait()

    half = pl.ds(pl.multiple_of(512 * core, 512), 512)
    other_half = pl.ds(pl.multiple_of(512 * (1 - core), 512), 512)
    wait_loads(3, 4)
    send(tm_v.at[:, other_half], tm_s, pair_sem.at[0], target["d"])
    send(hm_v, hm_s, pair_sem.at[1], target["d"])

    def product(low_turned, high):
        return mix_rate * lax.dot_general(
            low_turned, high, (((0,), (0,)), ((), ())), preferred_element_type=jnp.float32
        )

    row = sh * 320
    wait_loads(0, 1, 2)
    q_all[pl.ds(pl.multiple_of(row, 64), 320)] = (
        tq_v[...].astype(jnp.float32) + product(lq_v[...], hq_v[...])
    ).astype(jnp.bfloat16)
    wait_loads(12, 13)
    n_at = (x * 2 + core) * 4 + z
    n_all[n_at, y] = jnp.zeros((1, 128), jnp.float32)
    n_all[n_at, y, :, 0:40] = n1_v[...] + n2_v[...]
    for link, item in first:
        dispatch(link, item, place(own, core, item[-1]), own)
    wait_loads(6, 7, 8, 9, 10, 11)
    k_all[pl.ds(pl.multiple_of(row, 64), 320)] = (
        tk_v[...].astype(jnp.float32) + product(lk_v[...], hk_v[...])
    ).astype(jnp.bfloat16)
    v_all[pl.ds(pl.multiple_of(row, 64), 320)] = (
        tv_v[...].astype(jnp.float32) + product(lv_v[...], hv_v[...])
    ).astype(jnp.bfloat16)
    for k in (1, 2, 3):
        send(n_all.at[n_at, y], n_all.at[n_at, y], norm_sem.at[k - 1], device(dy=k))
    for link, item in second:
        dispatch(link, item, place(own, core, item[-1]), own)

    wait_loads(5)
    arrived(tm_s, pair_sem.at[0])
    arrived(hm_s, pair_sem.at[1])
    mine = pl.ds(pl.multiple_of(320 * core, 64), 320)
    others = pl.ds(pl.multiple_of(320 * (1 - core), 64), 320)
    low_half = lm_v[:, half]
    own_half = tm_v[:, half]
    for b in range(4):
        cols = slice(M_ROWS * b, M_ROWS * (b + 1))
        low = low_half[:, cols]
        turn[b, mine] = own_half[:, cols].astype(jnp.float32) + product(hm_v[...], low)
        turn[b, others] = tm_s[:, cols].astype(jnp.float32) + product(hm_s[...], low)
        rows = pl.ds(pl.multiple_of(512 * core + M_ROWS * b, M_ROWS), M_ROWS)
        m_all[own, rows] = turn[b].T.astype(jnp.bfloat16)
    for link, item in third:
        dispatch(link, item, place(own, core, item[-1]), own)

    for event in order:
        kind, chunk = event[0], event[-1]
        if kind == "ny":
            for k in (1, 2, 3):
                arrived(n_all.at[n_at, lax.rem(y + 4 - k, 4)], norm_sem.at[k - 1])
            for k in (1, 2, 3):
                send(n_all.at[n_at], n_all.at[n_at], norm_sem.at[3 + k - 1], device(dz=k))
        elif kind == "nz":
            block = (x * 2 + core) * 4
            for k in (1, 2, 3):
                arrived(n_all.at[block + lax.rem(z + 4 - k, 4)], norm_sem.at[3 + k - 1])
            line = n_all.at[pl.ds(block, 4)]
            for k in (1, 2, 3):
                send(line, line, norm_sem.at[6 + k - 1], device(dx=k))
            send(line, line, norm_sem.at[9], target["d"])
        elif kind == "nx":
            for k in (1, 2, 3):
                line = n_all.at[pl.ds((lax.rem(x + 4 - k, 4) * 2 + core) * 4, 4)]
                arrived(line, norm_sem.at[6 + k - 1])
                send(line, line, norm_sem.at[9 + k], target["d"])
        elif kind in ("r+", "r-"):
            way = HALF[chunk]
            src = relay_place(way, event[1], chunk)
            arrived(src, relay_sem.at[relay_index(way, event[1], chunk)])
            from_z = lax.rem(z + (3 if way == 0 else 1), 4)
            chip = (from_z // 2) * 4 + lax.rem(x + event[1], 4)
            for link, item in react(event):
                dispatch(link, item, src, chip)
        else:
            dz, dx = (1, event[1]) if kind == "z" else (event[1], event[2])
            chip = chip_at(dz, dx)
            src = place(chip, core, chunk)
            arrived(src, arrive_sem.at[arrive_index(dz, dx, chunk)])
            for link, item in react(event):
                dispatch(link, item, src, chip)

    for dz in (0, 1):
        for dx in range(4):
            for chunk in range(N_CHUNKS):
                arrived(place(chip_at(dz, dx), 1 - core, chunk), sib_sem.at[arrive_index(dz, dx, chunk)])
    for k in range(4):
        line = n_all.at[pl.ds((lax.rem(x + 4 - k, 4) * 2 + 1 - core) * 4, 4)]
        arrived(line, norm_sem.at[9 + k])
    for copy in started:
        copy.wait_send()


def write_kernel(q_all, k_all, v_all, m_all, n_all, q_out, k_out, v_out, m_out, n_out, lines, sems):
    copies = []
    for k in range(8):
        copies.append((m_all.at[k], m_out.at[:, pl.ds(640 * k, 640)]))
        copies.append((q_all.at[pl.ds(640 * k, 640)], q_out.at[pl.ds(640 * k, 640)]))
    copies += [(k_all, k_out), (v_all, v_out)]
    copies = [pltpu.make_async_copy(src, dst, sems.at[k]) for k, (src, dst) in enumerate(copies)]
    for copy in copies:
        copy.start()
    lane = lax.broadcasted_iota(jnp.int32, (8, 128), 1)
    acc = [jnp.zeros((8, 128), jnp.float32) for _ in range(5)]
    for i in range(16):
        core, zl, y = i // 8, (i // 4) % 2, i % 4
        rows = [n_all[(xx * 2 + core) * 4 + zh * 2 + zl, y] for zh in range(2) for xx in range(4)]
        block = jnp.concatenate(rows, axis=0)
        q, off = (40 * i) // 128, (40 * i) % 128
        turned = pltpu.roll(block, off, 1) if off else block
        acc[q] = jnp.where((lane >= off) & (lane < off + 40), turned, acc[q])
        if off + 40 > 128:
            acc[q + 1] = jnp.where(lane < off + 40 - 128, turned, acc[q + 1])
    for q in range(5):
        lines[pl.ds(q, 8, stride=5), :] = acc[q]
    n_out[...] = lines[...].astype(jnp.bfloat16)
    for copy in copies:
        copy.wait()


def body(
    train_query, low_query, high_query, train_key, low_key, high_key, train_value, low_value, high_value,
    train_mixed, low_mixed, high_mixed, norm_train, norm_step,
):
    bf16, f32 = jnp.bfloat16, jnp.float32
    args = (
        train_query, low_query.T, high_query, train_key, low_key.T, high_key, train_value, low_value.T, high_value,
        train_mixed.T, low_mixed.T, high_mixed, norm_train.reshape(1, -1), norm_step.reshape(1, -1),
    )
    vmem = pltpu.MemorySpace.VMEM
    q_all, k_all, v_all, m_all, n_all = pl.pallas_call(
        gather_kernel,
        name="gather",
        out_shape=[
            vmem((5120, 1024), bf16), vmem((5120, 128), bf16), vmem((5120, 128), bf16),
            vmem((8, 1024, 640), bf16), vmem((32, 4, 1, 128), f32),
        ],
        in_specs=[pl.BlockSpec(memory_space=pltpu.MemorySpace.HBM)] * 14,
        out_specs=[pl.BlockSpec(memory_space=vmem)] * 5,
        scratch_shapes=[pltpu.VMEM(a.shape, a.dtype) for a in args] + [
            pltpu.VMEM((320, 512), bf16), pltpu.VMEM((32, 320), bf16), pltpu.VMEM((4, 640, 128), f32),
            pltpu.VMEM((2, 160, 1024), bf16), pltpu.VMEM((2, 320, 128), bf16), pltpu.VMEM((2, 4, 256, 640), bf16),
            pltpu.SemaphoreType.DMA((N_LOADS,)), pltpu.SemaphoreType.DMA((N_SENDS,)),
            pltpu.SemaphoreType.DMA((80,)), pltpu.SemaphoreType.DMA((22,)), pltpu.SemaphoreType.DMA((80,)),
            pltpu.SemaphoreType.DMA((2,)), pltpu.SemaphoreType.DMA((13,)),
        ],
        compiler_params=pltpu.CompilerParams(
            collective_id=0, has_side_effects=True, vmem_limit_bytes=36 * 1024 * 1024
        ),
    )(*args)
    hbm = pltpu.MemorySpace.HBM
    q, k, v, m, n = pl.pallas_call(
        write_kernel,
        name="write",
        out_shape=[
            jax.ShapeDtypeStruct((5120, 1024), bf16), jax.ShapeDtypeStruct((5120, 128), bf16),
            jax.ShapeDtypeStruct((5120, 128), bf16), jax.ShapeDtypeStruct((1024, 5120), bf16),
            jax.ShapeDtypeStruct((40, 128), bf16),
        ],
        in_specs=[pl.BlockSpec(memory_space=vmem)] * 5,
        out_specs=[pl.BlockSpec(memory_space=hbm)] * 4 + [pl.BlockSpec(memory_space=vmem)],
        scratch_shapes=[pltpu.VMEM((40, 128), f32), pltpu.SemaphoreType.DMA((18,))],
        compiler_params=pltpu.CompilerParams(vmem_limit_bytes=2 * 1024 * 1024),
    )(q_all, k_all, v_all, m_all, n_all)
    return q, k, v, m, n.reshape(5120)


def solution(mesh):
    return jax.shard_map(
        body,
        mesh=mesh,
        in_specs=(
            P("shard", "tp"), P("shard", None), P(None, "tp"),
            P("shard", "tp"), P("shard", None), P(None, "tp"),
            P("shard", "tp"), P("shard", None), P(None, "tp"),
            P("tp", "shard"), P("tp", None), P(None, "shard"),
            P(("shard", "tp")), P(("shard", "tp")),
        ),
        out_specs=(P(None, "tp"), P(None, "tp"), P(None, "tp"), P("tp", None), P()),
        check_vma=False,
    )
```

```python
import functools
import heapq

import jax
import jax.numpy as jnp
from jax import lax
from jax.experimental import pallas as pl
from jax.experimental.pallas import tpu as pltpu
from jax.sharding import PartitionSpec as P

MESH = pl.DeviceIdType.MESH
mix_rate = 0.5

Q_ROWS = 80
M_ROWS = 128
HALF = (0, 0, 0, 1, 1, 1, 0, 0, 1, 1)
IS_B = (0,) * 6 + (1,) * 4
SIZES = (163840, 163840, 81920, 163840, 163840, 81920) + (163840,) * 4
N_CHUNKS = 10
KIND = (0, 0, 1, 0, 0, 2, 3, 3, 3, 3)


def own_sends(chunk, along_x, along_z):
    sends = []
    if along_z:
        sends.append(("z", ("z", 0, chunk)))
    if along_x:
        sends += [("x+", ("x+", 0, 3, chunk)), ("x-", ("x-", 0, 1, chunk))]
    if along_z:
        sends.append(("d", ("d", 0, 0, chunk)))
    return sends


def react(event):
    kind = event[0]
    if kind == "z":
        _, dx, chunk = event
        sends = [("d", ("d", 1, dx, chunk))]
        if not IS_B[chunk]:
            sends += [("x+", ("x+", 1, 3, chunk)), ("x-", ("x-", 1, 1, chunk))]
        return sends
    _, dz, dx, chunk = event
    sends = []
    if kind == "x+" and dx == 3 and HALF[chunk] == 0:
        sends.append(("x+", ("x+", dz, 2, chunk)))
    if kind == "x-" and dx == 1 and HALF[chunk] == 1:
        sends.append(("x-", ("x-", dz, 2, chunk)))
    if IS_B[chunk] and dz == 0:
        sends.append(("z", ("z", dx, chunk)))
    sends.append(("d", ("d", dz, dx, chunk)))
    return sends


def plan():
    first = []
    for chunk in (0, 3):
        first += own_sends(chunk, True, True)
    second = []
    for chunk in (1, 4, 2, 5):
        second += own_sends(chunk, False, True)
    third = []
    for chunk in (6, 8, 7, 9):
        third += own_sends(chunk, True, True)
    for chunk in (1, 4, 2, 5):
        third += own_sends(chunk, True, False)
    starts = [(2.0, first), (2.1, second), (6.0, third)]
    heap, count, free, order = [], 0, {}, []
    for time, sends in starts:
        heapq.heappush(heap, (time, count, None, sends))
        count += 1
    while heap:
        time, _, event, sends = heapq.heappop(heap)
        if event is not None:
            order.append((time, event))
            sends = react(event)
        for link, item in sends:
            if link == "d":
                continue
            done = max(time, free.get(link, 0.0)) + SIZES[item[-1]] / 45000.0
            free[link] = done
            heapq.heappush(heap, (done + 1.9, count, item, None))
            count += 1
    order += [(9.0, ("ny",)), (32.0, ("nz",)), (56.0, ("nx",))]
    order = [event for _, event in sorted(order, key=lambda pair: pair[0])]
    return first, second, third, order


N_LOADS = 14


def gather_kernel(
    tq, lq, hq, tk, lk, hk, tv, lv, hv, tm, lm, hm, n1, n2,
    q_all, k_all, v_all, m_all, n_all,
    tq_v, lq_v, hq_v, tk_v, lk_v, hk_v, tv_v, lv_v, hv_v, tm_v, lm_v, hm_v, n1_v, n2_v,
    tm_s, hm_s, turn,
    load_sem, send_sem, arrive_sem, sib_sem, pair_sem, norm_sem,
):
    sh = lax.axis_index("shard")
    tp = lax.axis_index("tp")
    core = lax.rem(sh, 2)
    x = lax.rem(sh // 2, 4)
    z = (sh // 8) * 2 + tp // 4
    y = lax.rem(tp, 4)

    def device(dx=0, dz=0, dy=0, other=False):
        zz = lax.rem(z + dz, 4)
        cc = 1 - core if other else core
        return (
            ((zz // 2) * 4 + lax.rem(x + dx, 4)) * 2 + cc,
            lax.rem(zz, 2) * 4 + lax.rem(y + dy, 4),
        )

    target = {
        "x+": device(dx=1), "x-": device(dx=3), "z": device(dz=2), "d": device(other=True),
    }

    partners = [device(dx=k) for k in (1, 2, 3)] + [device(dz=k) for k in (1, 2, 3)]
    partners += [device(dy=k) for k in (1, 2, 3)] + [device(other=True)]
    barrier = pltpu.get_barrier_semaphore()
    for partner in partners:
        pl.semaphore_signal(barrier, inc=1, device_id=partner, device_id_type=MESH)

    loads = []
    for k, (src, dst) in enumerate((
        (tq, tq_v), (lq, lq_v), (hq, hq_v), (tm, tm_v), (hm, hm_v), (lm, lm_v), (tk, tk_v), (lk, lk_v), (hk, hk_v),
        (tv, tv_v), (lv, lv_v), (hv, hv_v), (n1, n1_v), (n2, n2_v),
    )):
        copy = pltpu.make_async_copy(src, dst, load_sem.at[k])
        copy.start()
        loads.append(copy)

    def send(src, dst, sent, sem, to):
        copy = pltpu.make_async_remote_copy(
            src_ref=src, dst_ref=dst, send_sem=sent, recv_sem=sem, device_id=to, device_id_type=MESH,
        )
        copy.start()
        return copy

    def waiting(ref, sent, sem):
        return pltpu.make_async_remote_copy(
            src_ref=ref, dst_ref=ref, send_sem=sent, recv_sem=sem, device_id=target["d"], device_id_type=MESH,
        )

    def arrived(dst, sem):
        waiting(dst, send_sem.at[0], sem).wait_recv()

    n_sent = [[0, 0] for _ in range(4)]

    def many(kind, count):
        if kind == 0:
            return q_all.at[pl.ds(0, Q_ROWS * count)]
        if kind < 3:
            return (k_all if kind == 1 else v_all).at[pl.ds(0, 320 * count)]
        if count % 8 == 0:
            return m_all.at[pl.ds(0, count // 8)]
        return m_all.at[pl.ds(0, count // 4), pl.ds(0, 512)]

    def place(chip, cc, chunk):
        row = (chip * 2 + cc) * 320
        if chunk in (2, 5):
            return (k_all if chunk == 2 else v_all).at[pl.ds(pl.multiple_of(row, 64), 320)]
        if chunk < 6:
            part = chunk if chunk < 2 else chunk - 1
            return q_all.at[pl.ds(pl.multiple_of(row + Q_ROWS * part, 16), Q_ROWS)]
        return m_all.at[chip, pl.ds(pl.multiple_of(512 * cc + M_ROWS * (chunk - 6), M_ROWS), M_ROWS)]

    def chip_at(dz2, dx):
        return (lax.rem(sh // 8 + dz2, 2)) * 4 + lax.rem(x + dx, 4)

    def arrive_index(dz, dx, chunk):
        return (dz * 4 + dx) * N_CHUNKS + chunk

    def dispatch(link, item, src, chip):
        kind, chunk = KIND[item[-1]], item[-1]
        if link == "d":
            sem, side = sib_sem.at[kind], 1
        else:
            dz, dx = (1, item[1]) if link == "z" else (item[1], item[2])
            sem, side = arrive_sem.at[arrive_index(dz, dx, chunk)], 0
        n_sent[kind][side] += 1
        send(src, src, send_sem.at[kind * 2 + side], sem, target[link])

    first, second, third, order = plan()
    own = chip_at(0, 0)

    def wait_loads(*which):
        for k in which:
            loads[k].wait()

    def product(low_turned, high):
        return mix_rate * lax.dot_general(
            low_turned, high, (((0,), (0,)), ((), ())), preferred_element_type=jnp.float32
        )

    row = sh * 320
    wait_loads(0, 1, 2)
    q_all[pl.ds(pl.multiple_of(row, 64), 320)] = (
        tq_v[...].astype(jnp.float32) + product(lq_v[...], hq_v[...])
    ).astype(jnp.bfloat16)
    wait_loads(6, 7, 8, 9, 10, 11)
    k_all[pl.ds(pl.multiple_of(row, 64), 320)] = (
        tk_v[...].astype(jnp.float32) + product(lk_v[...], hk_v[...])
    ).astype(jnp.bfloat16)
    v_all[pl.ds(pl.multiple_of(row, 64), 320)] = (
        tv_v[...].astype(jnp.float32) + product(lv_v[...], hv_v[...])
    ).astype(jnp.bfloat16)
    wait_loads(12, 13)
    n_at = (x * 2 + core) * 4 + z
    n_all[n_at, y] = jnp.zeros((1, 128), jnp.float32)
    n_all[n_at, y, :, 0:40] = n1_v[...] + n2_v[...]
    wait_loads(3, 4, 5)
    pl.semaphore_wait(barrier, len(partners))

    half = pl.ds(pl.multiple_of(512 * core, 512), 512)
    other_half = pl.ds(pl.multiple_of(512 * (1 - core), 512), 512)
    small = [
        send(tm_v.at[:, other_half], tm_s, pair_sem.at[2], pair_sem.at[0], target["d"]),
        send(hm_v, hm_s, pair_sem.at[3], pair_sem.at[1], target["d"]),
    ]
    for link, item in first:
        dispatch(link, item, place(own, core, item[-1]), own)
    for k in (1, 2, 3):
        line = n_all.at[n_at, y]
        small.append(send(line, line, norm_sem.at[12 + k], norm_sem.at[k - 1], device(dy=k)))
    for link, item in second:
        dispatch(link, item, place(own, core, item[-1]), own)

    arrived(tm_s, pair_sem.at[0])
    arrived(hm_s, pair_sem.at[1])
    mine = pl.ds(pl.multiple_of(320 * core, 64), 320)
    others = pl.ds(pl.multiple_of(320 * (1 - core), 64), 320)
    low_half = lm_v[:, half]
    own_half = tm_v[:, half]
    for b in range(4):
        cols = slice(M_ROWS * b, M_ROWS * (b + 1))
        low = low_half[:, cols]
        turn[b, mine] = own_half[:, cols].astype(jnp.float32) + product(hm_v[...], low)
        turn[b, others] = tm_s[:, cols].astype(jnp.float32) + product(hm_s[...], low)
        rows = pl.ds(pl.multiple_of(512 * core + M_ROWS * b, M_ROWS), M_ROWS)
        m_all[own, rows] = turn[b].T.astype(jnp.bfloat16)
    for link, item in third:
        dispatch(link, item, place(own, core, item[-1]), own)

    for event in order:
        kind, chunk = event[0], event[-1]
        if kind == "ny":
            for k in (1, 2, 3):
                arrived(n_all.at[n_at, lax.rem(y + 4 - k, 4)], norm_sem.at[k - 1])
            for k in (1, 2, 3):
                line = n_all.at[n_at]
                small.append(send(line, line, norm_sem.at[15 + k], norm_sem.at[3 + k - 1], device(dz=k)))
        elif kind == "nz":
            block = (x * 2 + core) * 4
            for k in (1, 2, 3):
                arrived(n_all.at[block + lax.rem(z + 4 - k, 4)], norm_sem.at[3 + k - 1])
            line = n_all.at[pl.ds(block, 4)]
            for k in (1, 2, 3):
                small.append(send(line, line, norm_sem.at[18 + k], norm_sem.at[6 + k - 1], device(dx=k)))
            small.append(send(line, line, norm_sem.at[22], norm_sem.at[9], target["d"]))
        elif kind == "nx":
            for k in (1, 2, 3):
                line = n_all.at[pl.ds((lax.rem(x + 4 - k, 4) * 2 + core) * 4, 4)]
                arrived(line, norm_sem.at[6 + k - 1])
                small.append(send(line, line, norm_sem.at[22 + k], norm_sem.at[9 + k], target["d"]))
        else:
            dz, dx = (1, event[1]) if kind == "z" else (event[1], event[2])
            chip = chip_at(dz, dx)
            src = place(chip, core, chunk)
            arrived(src, arrive_sem.at[arrive_index(dz, dx, chunk)])
            for link, item in react(event):
                dispatch(link, item, src, chip)

    for k in range(4):
        line = n_all.at[pl.ds((lax.rem(x + 4 - k, 4) * 2 + 1 - core) * 4, 4)]
        arrived(line, norm_sem.at[9 + k])
    for copy in small:
        copy.wait_send()
    for kind, per_piece in enumerate((4, 1, 1, 4)):
        for side in (0, 1):
            count = n_sent[kind][side]
            waiting(many(kind, count), send_sem.at[kind * 2 + side], sib_sem.at[0]).wait_send()
        arrived(many(kind, per_piece * 8), sib_sem.at[kind])


def write_kernel(q_all, k_all, v_all, m_all, n_all, q_out, k_out, v_out, m_out, n_out, lines, rounded, sems):
    copies = []
    for k in range(8):
        copies.append((m_all.at[k], m_out.at[:, pl.ds(640 * k, 640)]))
        copies.append((q_all.at[pl.ds(640 * k, 640)], q_out.at[pl.ds(640 * k, 640)]))
    copies += [(k_all, k_out), (v_all, v_out)]
    copies = [pltpu.make_async_copy(src, dst, sems.at[k]) for k, (src, dst) in enumerate(copies)]
    for copy in copies:
        copy.start()
    lane = lax.broadcasted_iota(jnp.int32, (8, 128), 1)
    acc = [jnp.zeros((8, 128), jnp.float32) for _ in range(5)]
    for i in range(16):
        core, zl, y = i // 8, (i // 4) % 2, i % 4
        rows = [n_all[(xx * 2 + core) * 4 + zh * 2 + zl, y] for zh in range(2) for xx in range(4)]
        block = jnp.concatenate(rows, axis=0)
        q, off = (40 * i) // 128, (40 * i) % 128
        turned = pltpu.roll(block, off, 1) if off else block
        acc[q] = jnp.where((lane >= off) & (lane < off + 40), turned, acc[q])
        if off + 40 > 128:
            acc[q + 1] = jnp.where(lane < off + 40 - 128, turned, acc[q + 1])
    for q in range(5):
        lines[pl.ds(q, 8, stride=5), :] = acc[q]
    rounded[...] = lines[...].astype(jnp.bfloat16)
    last = pltpu.make_async_copy(rounded, n_out, sems.at[len(copies)])
    last.start()
    copies.append(last)
    for copy in copies:
        copy.wait()


def body(
    train_query, low_query, high_query, train_key, low_key, high_key, train_value, low_value, high_value,
    train_mixed, low_mixed, high_mixed, norm_train, norm_step,
):
    bf16, f32 = jnp.bfloat16, jnp.float32
    args = (
        train_query, low_query.T, high_query, train_key, low_key.T, high_key, train_value, low_value.T, high_value,
        train_mixed.T, low_mixed.T, high_mixed, norm_train.reshape(1, -1), norm_step.reshape(1, -1),
    )
    vmem = pltpu.MemorySpace.VMEM
    q_all, k_all, v_all, m_all, n_all = pl.pallas_call(
        gather_kernel,
        name="gather",
        out_shape=[
            vmem((5120, 1024), bf16), vmem((5120, 128), bf16), vmem((5120, 128), bf16),
            vmem((8, 1024, 640), bf16), vmem((32, 4, 1, 128), f32),
        ],
        in_specs=[pl.BlockSpec(memory_space=pltpu.MemorySpace.HBM)] * 14,
        out_specs=[pl.BlockSpec(memory_space=vmem)] * 5,
        scratch_shapes=[pltpu.VMEM(a.shape, a.dtype) for a in args] + [
            pltpu.VMEM((320, 512), bf16), pltpu.VMEM((32, 320), bf16), pltpu.VMEM((4, 640, 128), f32),
            pltpu.SemaphoreType.DMA((N_LOADS,)), pltpu.SemaphoreType.DMA((8,)),
            pltpu.SemaphoreType.DMA((80,)), pltpu.SemaphoreType.DMA((4,)),
            pltpu.SemaphoreType.DMA((4,)), pltpu.SemaphoreType.DMA((26,)),
        ],
        compiler_params=pltpu.CompilerParams(
            collective_id=0, has_side_effects=True, vmem_limit_bytes=36 * 1024 * 1024
        ),
    )(*args)
    hbm = pltpu.MemorySpace.HBM
    q, k, v, m, n = pl.pallas_call(
        write_kernel,
        name="write",
        out_shape=[
            jax.ShapeDtypeStruct((5120, 1024), bf16), jax.ShapeDtypeStruct((5120, 128), bf16),
            jax.ShapeDtypeStruct((5120, 128), bf16), jax.ShapeDtypeStruct((1024, 5120), bf16),
            jax.ShapeDtypeStruct((40, 128), bf16),
        ],
        in_specs=[pl.BlockSpec(memory_space=vmem)] * 5,
        out_specs=[pl.BlockSpec(memory_space=hbm)] * 5,
        scratch_shapes=[pltpu.VMEM((40, 128), f32), pltpu.VMEM((40, 128), bf16), pltpu.SemaphoreType.DMA((19,))],
        compiler_params=pltpu.CompilerParams(vmem_limit_bytes=2 * 1024 * 1024),
    )(q_all, k_all, v_all, m_all, n_all)
    return q, k, v, m, n.reshape(5120)


def solution(mesh):
    return jax.shard_map(
        body,
        mesh=mesh,
        in_specs=(
            P("shard", "tp"), P("shard", None), P(None, "tp"),
            P("shard", "tp"), P("shard", None), P(None, "tp"),
            P("shard", "tp"), P("shard", None), P(None, "tp"),
            P("tp", "shard"), P("tp", None), P(None, "shard"),
            P(("shard", "tp")), P(("shard", "tp")),
        ),
        out_specs=(P(None, "tp"), P(None, "tp"), P(None, "tp"), P("tp", None), P()),
        check_vma=False,
    )
```

```python
import functools
import heapq

import jax
import jax.numpy as jnp
from jax import lax
from jax.experimental import pallas as pl
from jax.experimental.pallas import tpu as pltpu
from jax.sharding import PartitionSpec as P

MESH = pl.DeviceIdType.MESH
mix_rate = 0.5

Q_ROWS = 160
M_ROWS = 256
HALF = (0, 0, 1, 1, 0, 1)
IS_B = (0, 0, 0, 0, 1, 1)
KIND = (0, 1, 0, 2, 3, 3)
SIZES = (327680, 81920, 327680, 81920, 327680, 327680)
N_CHUNKS = 6


def own_sends(chunk, along_x, along_z):
    sends = []
    if along_z:
        sends.append(("z", ("z", 0, chunk)))
    if along_x:
        sends += [("x+", ("x+", 0, 3, chunk)), ("x-", ("x-", 0, 1, chunk))]
    if along_z:
        sends.append(("d", ("d", 0, 0, chunk)))
    return sends


def react(event):
    kind = event[0]
    if kind == "z":
        _, dx, chunk = event
        sends = [("d", ("d", 1, dx, chunk))]
        if not IS_B[chunk]:
            sends += [("x+", ("x+", 1, 3, chunk)), ("x-", ("x-", 1, 1, chunk))]
        return sends
    _, dz, dx, chunk = event
    sends = []
    if kind == "x+" and dx == 3 and HALF[chunk] == 0:
        sends.append(("x+", ("x+", dz, 2, chunk)))
    if kind == "x-" and dx == 1 and HALF[chunk] == 1:
        sends.append(("x-", ("x-", dz, 2, chunk)))
    if IS_B[chunk] and dz == 0:
        sends.append(("z", ("z", dx, chunk)))
    sends.append(("d", ("d", dz, dx, chunk)))
    return sends


def plan():
    first = []
    for chunk in (0,):
        first += own_sends(chunk, True, True)
    second = []
    for chunk in (2, 1, 3):
        second += own_sends(chunk, False, True)
    third = []
    for chunk in (4, 5):
        third += own_sends(chunk, True, True)
    for chunk in (2, 1, 3):
        third += own_sends(chunk, True, False)
    starts = [(2.0, first), (2.2, second), (5.5, third)]
    heap, count, free, order = [], 0, {}, []
    for time, sends in starts:
        heapq.heappush(heap, (time, count, None, sends))
        count += 1
    while heap:
        time, _, event, sends = heapq.heappop(heap)
        if event is not None:
            order.append((time, event))
            sends = react(event)
        for link, item in sends:
            if link == "d":
                continue
            done = max(time, free.get(link, 0.0)) + SIZES[item[-1]] / 45000.0
            free[link] = done
            heapq.heappush(heap, (done + 1.9, count, item, None))
            count += 1
    order += [(t, (name,)) for t, name in ((9.0, "n0"), (38.0, "n1"), (64.0, "n2"), (67.5, "n3"), (71.0, "n4"), (74.0, "n5"))]
    order = [event for _, event in sorted(order, key=lambda pair: pair[0])]
    return first, second, third, order


N_LOADS = 14


def gather_kernel(
    tq, lq, hq, tk, lk, hk, tv, lv, hv, tm, lm, hm, n1, n2,
    q_all, k_all, v_all, m_all, n_all,
    tq_v, lq_v, hq_v, tk_v, lk_v, hk_v, tv_v, lv_v, hv_v, tm_v, lm_v, hm_v, n1_v, n2_v,
    tm_s, hm_s, turn,
    load_sem, send_sem, arrive_sem, sib_sem, pair_sem, norm_sem,
):
    sh = lax.axis_index("shard")
    tp = lax.axis_index("tp")
    core = lax.rem(sh, 2)
    x = lax.rem(sh // 2, 4)
    z = (sh // 8) * 2 + tp // 4
    y = lax.rem(tp, 4)

    def device(dx=0, dz=0, dy=0, other=False):
        zz = lax.rem(z + dz, 4)
        cc = 1 - core if other else core
        return (
            ((zz // 2) * 4 + lax.rem(x + dx, 4)) * 2 + cc,
            lax.rem(zz, 2) * 4 + lax.rem(y + dy, 4),
        )

    target = {
        "x+": device(dx=1), "x-": device(dx=3), "z": device(dz=2), "d": device(other=True),
    }

    beside = device(dz=1 + 2 * lax.rem(z, 2))
    partners = [device(dx=k) for k in (1, 2, 3)] + [beside, target["z"]]
    partners += [device(dy=k) for k in (1, 3)] + [target["d"]]
    barrier = pltpu.get_barrier_semaphore()
    for partner in partners:
        pl.semaphore_signal(barrier, inc=1, device_id=partner, device_id_type=MESH)

    loads = []
    for k, (src, dst) in enumerate((
        (tq, tq_v), (lq, lq_v), (hq, hq_v), (tm, tm_v), (hm, hm_v), (lm, lm_v), (tk, tk_v), (lk, lk_v), (hk, hk_v),
        (tv, tv_v), (lv, lv_v), (hv, hv_v), (n1, n1_v), (n2, n2_v),
    )):
        copy = pltpu.make_async_copy(src, dst, load_sem.at[k])
        copy.start()
        loads.append(copy)

    def send(src, dst, sent, sem, to):
        copy = pltpu.make_async_remote_copy(
            src_ref=src, dst_ref=dst, send_sem=sent, recv_sem=sem, device_id=to, device_id_type=MESH,
        )
        copy.start()
        return copy

    def waiting(ref, sent, sem):
        return pltpu.make_async_remote_copy(
            src_ref=ref, dst_ref=ref, send_sem=sent, recv_sem=sem, device_id=target["d"], device_id_type=MESH,
        )

    def arrived(dst, sem):
        waiting(dst, send_sem.at[0], sem).wait_recv()

    n_sent = [[0, 0] for _ in range(4)]

    def many(kind, count):
        if kind == 0:
            return q_all.at[pl.ds(0, Q_ROWS * count)]
        if kind < 3:
            return (k_all if kind == 1 else v_all).at[pl.ds(0, 320 * count)]
        if count % 4 == 0:
            return m_all.at[pl.ds(0, count // 4)]
        return m_all.at[pl.ds(0, count // 2), pl.ds(0, 512)]

    def place(chip, cc, chunk):
        row = (chip * 2 + cc) * 320
        if KIND[chunk] in (1, 2):
            return (k_all if KIND[chunk] == 1 else v_all).at[pl.ds(pl.multiple_of(row, 64), 320)]
        if KIND[chunk] == 0:
            return q_all.at[pl.ds(pl.multiple_of(row + Q_ROWS * HALF[chunk], 32), Q_ROWS)]
        return m_all.at[chip, pl.ds(pl.multiple_of(512 * cc + M_ROWS * HALF[chunk], M_ROWS), M_ROWS)]

    def chip_at(dz2, dx):
        return (lax.rem(sh // 8 + dz2, 2)) * 4 + lax.rem(x + dx, 4)

    def arrive_index(dz, dx, chunk):
        return (dz * 4 + dx) * N_CHUNKS + chunk

    def dispatch(link, item, src, chip):
        kind, chunk = KIND[item[-1]], item[-1]
        if link == "d":
            sem, side = sib_sem.at[kind], 1
        else:
            dz, dx = (1, item[1]) if link == "z" else (item[1], item[2])
            sem, side = arrive_sem.at[arrive_index(dz, dx, chunk)], 0
        n_sent[kind][side] += 1
        send(src, src, send_sem.at[kind * 2 + side], sem, target[link])

    first, second, third, order = plan()
    own = chip_at(0, 0)

    def wait_loads(*which):
        for k in which:
            loads[k].wait()

    def product(low_turned, high):
        return mix_rate * lax.dot_general(
            low_turned, high, (((0,), (0,)), ((), ())), preferred_element_type=jnp.float32
        )

    row = sh * 320
    wait_loads(12, 13)
    plane = core * 4 + y
    n_all[plane, z, x] = jnp.zeros((1, 128), jnp.float32)
    n_all[plane, z, x, :, 0:40] = n1_v[...] + n2_v[...]
    wait_loads(0, 1, 2)
    q_all[pl.ds(pl.multiple_of(row, 64), 320)] = (
        tq_v[...].astype(jnp.float32) + product(lq_v[...], hq_v[...])
    ).astype(jnp.bfloat16)
    pl.semaphore_wait(barrier, len(partners))
    line = n_all.at[plane, z, x]
    small = [send(line, line, norm_sem.at[8 + k], norm_sem.at[k - 1], device(dx=k)) for k in (1, 2, 3)]
    for link, item in first:
        dispatch(link, item, place(own, core, item[-1]), own)

    half = pl.ds(pl.multiple_of(512 * core, 512), 512)
    other_half = pl.ds(pl.multiple_of(512 * (1 - core), 512), 512)
    wait_loads(3, 4)
    small += [
        send(tm_v.at[:, other_half], tm_s, pair_sem.at[2], pair_sem.at[0], target["d"]),
        send(hm_v, hm_s, pair_sem.at[3], pair_sem.at[1], target["d"]),
    ]

    wait_loads(6, 7, 8, 9, 10, 11)
    k_all[pl.ds(pl.multiple_of(row, 64), 320)] = (
        tk_v[...].astype(jnp.float32) + product(lk_v[...], hk_v[...])
    ).astype(jnp.bfloat16)
    v_all[pl.ds(pl.multiple_of(row, 64), 320)] = (
        tv_v[...].astype(jnp.float32) + product(lv_v[...], hv_v[...])
    ).astype(jnp.bfloat16)
    for link, item in second:
        dispatch(link, item, place(own, core, item[-1]), own)

    wait_loads(5)
    arrived(tm_s, pair_sem.at[0])
    arrived(hm_s, pair_sem.at[1])
    mine = pl.ds(pl.multiple_of(320 * core, 64), 320)
    others = pl.ds(pl.multiple_of(320 * (1 - core), 64), 320)
    low_half = lm_v[:, half]
    own_half = tm_v[:, half]
    for b in range(4):
        cols = slice(128 * b, 128 * (b + 1))
        low = low_half[:, cols]
        turn[b, mine] = own_half[:, cols].astype(jnp.float32) + product(hm_v[...], low)
        turn[b, others] = tm_s[:, cols].astype(jnp.float32) + product(hm_s[...], low)
        rows = pl.ds(pl.multiple_of(512 * core + 128 * b, 128), 128)
        m_all[own, rows] = turn[b].T.astype(jnp.bfloat16)
    for link, item in third:
        dispatch(link, item, place(own, core, item[-1]), own)

    for event in order:
        kind, chunk = event[0], event[-1]
        if kind == "n0":
            for k in (1, 2, 3):
                arrived(n_all.at[plane, z, lax.rem(x + 4 - k, 4)], norm_sem.at[k - 1])
            line = n_all.at[plane, z]
            small.append(send(line, line, norm_sem.at[12], norm_sem.at[3], beside))
        elif kind == "n1":
            arrived(n_all.at[plane, lax.rem(z + 1 + 2 * lax.rem(z, 2), 4)], norm_sem.at[3])
            line = n_all.at[plane, pl.ds((z // 2) * 2, 2)]
            small.append(send(line, line, norm_sem.at[13], norm_sem.at[4], target["z"]))
        elif kind == "n2":
            arrived(n_all.at[plane, pl.ds((1 - z // 2) * 2, 2)], norm_sem.at[4])
            line = n_all.at[plane]
            for k in (1, 3):
                small.append(send(line, line, norm_sem.at[13 + k], norm_sem.at[4 + k], device(dy=k)))
        elif kind == "n3":
            for k in (1, 3):
                arrived(n_all.at[core * 4 + lax.rem(y + 4 - k, 4)], norm_sem.at[4 + k])
            line = n_all.at[core * 4 + lax.rem(y + 3, 4)]
            small.append(send(line, line, norm_sem.at[15], norm_sem.at[6], device(dy=1)))
        elif kind == "n4":
            arrived(n_all.at[core * 4 + lax.rem(y + 2, 4)], norm_sem.at[6])
            line = n_all.at[pl.ds(core * 4, 4)]
            small.append(send(line, line, norm_sem.at[17], norm_sem.at[8], target["d"]))
        elif kind == "n5":
            arrived(n_all.at[pl.ds((1 - core) * 4, 4)], norm_sem.at[8])
            for copy in small:
                copy.wait_send()
        else:
            dz, dx = (1, event[1]) if kind == "z" else (event[1], event[2])
            chip = chip_at(dz, dx)
            src = place(chip, core, chunk)
            arrived(src, arrive_sem.at[arrive_index(dz, dx, chunk)])
            for link, item in react(event):
                dispatch(link, item, src, chip)

    for kind, per_piece in enumerate((2, 1, 1, 2)):
        for side in (0, 1):
            count = n_sent[kind][side]
            waiting(many(kind, count), send_sem.at[kind * 2 + side], sib_sem.at[0]).wait_send()
        arrived(many(kind, per_piece * 8), sib_sem.at[kind])


def write_kernel(q_all, k_all, v_all, m_all, n_all, q_out, k_out, v_out, m_out, n_out, lines, rounded, sems):
    copies = []
    for k in range(8):
        copies.append((m_all.at[k], m_out.at[:, pl.ds(640 * k, 640)]))
        copies.append((q_all.at[pl.ds(640 * k, 640)], q_out.at[pl.ds(640 * k, 640)]))
    copies += [(k_all, k_out), (v_all, v_out)]
    copies = [pltpu.make_async_copy(src, dst, sems.at[k]) for k, (src, dst) in enumerate(copies)]
    for copy in copies:
        copy.start()
    lane = lax.broadcasted_iota(jnp.int32, (8, 128), 1)
    acc = [jnp.zeros((8, 128), jnp.float32) for _ in range(5)]
    for i in range(16):
        core, zl, y = i // 8, (i // 4) % 2, i % 4
        rows = [n_all[core * 4 + y, zh * 2 + zl, xx] for zh in range(2) for xx in range(4)]
        block = jnp.concatenate(rows, axis=0)
        q, off = (40 * i) // 128, (40 * i) % 128
        turned = pltpu.roll(block, off, 1) if off else block
        acc[q] = jnp.where((lane >= off) & (lane < off + 40), turned, acc[q])
        if off + 40 > 128:
            acc[q + 1] = jnp.where(lane < off + 40 - 128, turned, acc[q + 1])
    for q in range(5):
        lines[pl.ds(q, 8, stride=5), :] = acc[q]
    rounded[...] = lines[...].astype(jnp.bfloat16)
    last = pltpu.make_async_copy(rounded, n_out, sems.at[len(copies)])
    last.start()
    copies.append(last)
    for copy in copies:
        copy.wait()


def body(
    train_query, low_query, high_query, train_key, low_key, high_key, train_value, low_value, high_value,
    train_mixed, low_mixed, high_mixed, norm_train, norm_step,
):
    bf16, f32 = jnp.bfloat16, jnp.float32
    args = (
        train_query, low_query.T, high_query, train_key, low_key.T, high_key, train_value, low_value.T, high_value,
        train_mixed.T, low_mixed.T, high_mixed, norm_train.reshape(1, -1), norm_step.reshape(1, -1),
    )
    vmem = pltpu.MemorySpace.VMEM
    q_all, k_all, v_all, m_all, n_all = pl.pallas_call(
        gather_kernel,
        name="gather",
        out_shape=[
            vmem((5120, 1024), bf16), vmem((5120, 128), bf16), vmem((5120, 128), bf16),
            vmem((8, 1024, 640), bf16), vmem((8, 4, 4, 1, 128), f32),
        ],
        in_specs=[pl.BlockSpec(memory_space=pltpu.MemorySpace.HBM)] * 14,
        out_specs=[pl.BlockSpec(memory_space=vmem)] * 5,
        scratch_shapes=[pltpu.VMEM(a.shape, a.dtype) for a in args] + [
            pltpu.VMEM((320, 512), bf16), pltpu.VMEM((32, 320), bf16), pltpu.VMEM((4, 640, 128), f32),
            pltpu.SemaphoreType.DMA((N_LOADS,)), pltpu.SemaphoreType.DMA((8,)),
            pltpu.SemaphoreType.DMA((8 * N_CHUNKS,)), pltpu.SemaphoreType.DMA((4,)),
            pltpu.SemaphoreType.DMA((4,)), pltpu.SemaphoreType.DMA((18,)),
        ],
        compiler_params=pltpu.CompilerParams(
            collective_id=0, has_side_effects=True, vmem_limit_bytes=36 * 1024 * 1024
        ),
    )(*args)
    hbm = pltpu.MemorySpace.HBM
    q, k, v, m, n = pl.pallas_call(
        write_kernel,
        name="write",
        out_shape=[
            jax.ShapeDtypeStruct((5120, 1024), bf16), jax.ShapeDtypeStruct((5120, 128), bf16),
            jax.ShapeDtypeStruct((5120, 128), bf16), jax.ShapeDtypeStruct((1024, 5120), bf16),
            jax.ShapeDtypeStruct((40, 128), bf16),
        ],
        in_specs=[pl.BlockSpec(memory_space=vmem)] * 5,
        out_specs=[pl.BlockSpec(memory_space=hbm)] * 5,
        scratch_shapes=[pltpu.VMEM((40, 128), f32), pltpu.VMEM((40, 128), bf16), pltpu.SemaphoreType.DMA((19,))],
        compiler_params=pltpu.CompilerParams(vmem_limit_bytes=2 * 1024 * 1024),
    )(q_all, k_all, v_all, m_all, n_all)
    return q, k, v, m, n.reshape(5120)


def solution(mesh):
    return jax.shard_map(
        body,
        mesh=mesh,
        in_specs=(
            P("shard", "tp"), P("shard", None), P(None, "tp"),
            P("shard", "tp"), P("shard", None), P(None, "tp"),
            P("shard", "tp"), P("shard", None), P(None, "tp"),
            P("tp", "shard"), P("tp", None), P(None, "shard"),
            P(("shard", "tp")), P(("shard", "tp")),
        ),
        out_specs=(P(None, "tp"), P(None, "tp"), P(None, "tp"), P("tp", None), P()),
        check_vma=False,
    )
```

```python
import functools
import heapq

import jax
import jax.numpy as jnp
from jax import lax
from jax.experimental import pallas as pl
from jax.experimental.pallas import tpu as pltpu
from jax.sharding import PartitionSpec as P

MESH = pl.DeviceIdType.MESH
mix_rate = 0.5

Q_ROWS = 160
M_ROWS = 256
KIND = (0, 1, 0, 2, 3, 3, 0, 3, 3, 3)
FROM = (0, 0, 1, 0, 0, 1, 0, 0, 1, 1.75)
WEIGHT = (1, 1, 1, 1, 1, 1, 2, 2, 0.75, 0.25)
SIZES = (327680, 81920, 327680, 81920, 327680, 327680, 655360, 655360, 245760, 81920)
ONWARD = {"x+": {6: 0, 0: 0, 1: 1, 7: 4}, "x-": {6: 2, 2: 2, 3: 3, 7: 5}}
PARTNERS = {"x+": (0, 1, 2, 3), "x-": (2, 3, 0, 1)}


def own_sends(chunk, along_x, along_z):
    sends = []
    if along_z:
        sends.append(("z", ("z", 0, chunk)))
    if along_x:
        sends += [("x+", ("x+", 0, 3, chunk)), ("x-", ("x-", 0, 1, chunk))]
    if along_z:
        sends.append(("d", ("d", 0, 0, chunk)))
    return sends


def react(event):
    kind = event[0]
    if kind == "z":
        _, dx, chunk = event
        return [("d", ("d", 1, dx, chunk))]
    _, dz, dx, chunk = event
    sends = []
    if dx != 2 and chunk in ONWARD[kind]:
        sends.append((kind, (kind, dz, 2, ONWARD[kind][chunk])))
        if (dz, chunk) == (0, 7):
            sends += [(kind, (kind, 1, dx, other)) for other in PARTNERS[kind]]
    if KIND[chunk] == 3 and dz == 0:
        sends += [("z", ("z", dx, part)) for part in ((8, 9) if chunk == 5 else (chunk,))]
    sends.append(("d", ("d", dz, dx, chunk)))
    return sends


def plan():
    first = []
    for chunk in (6,):
        first += own_sends(chunk, True, True)
    second = []
    for chunk in (1, 3):
        second += own_sends(chunk, False, True)
    third = []
    for chunk in (7,):
        third += own_sends(chunk, True, True)
    for chunk in (1, 3):
        third += own_sends(chunk, True, False)
    starts = [(2.0, first), (2.2, second), (5.5, third)]
    heap, count, free, order = [], 0, {}, []
    for time, sends in starts:
        heapq.heappush(heap, (time, count, None, sends))
        count += 1
    while heap:
        time, _, event, sends = heapq.heappop(heap)
        if event is not None:
            order.append((time, event))
            sends = react(event)
        for link, item in sends:
            if link == "d":
                continue
            done = max(time, free.get(link, 0.0)) + SIZES[item[-1]] / 45000.0
            free[link] = done
            heapq.heappush(heap, (done + 1.9, count, item, None))
            count += 1
    order += [(t, (name,)) for t, name in ((9.0, "n0"), (38.0, "n1"), (64.0, "n2"), (67.5, "n3"), (71.0, "n4"), (74.0, "n5"))]
    order = [event for _, event in sorted(order, key=lambda pair: pair[0])]
    held = [order.index(("x+", 0, 3, 7)), order.index(("x-", 0, 1, 7))]
    assert min(held) > max(order.index(("z", 0, chunk)) for chunk in (6, 1, 3))
    return first, second, third, order


def slots():
    found = {}
    for event in plan()[3]:
        if event[0][0] != "n":
            dz, dx = (1, event[1]) if event[0] == "z" else (event[1], event[2])
            found[(dz, dx, event[-1])] = len(found)
    return found


SLOTS = slots()
N_LOADS = 14


def gather_kernel(
    tq, lq, hq, tk, lk, hk, tv, lv, hv, tm, lm, hm, n1, n2,
    q_all, k_all, v_all, m_all, n_all,
    tq_v, lq_v, hq_v, tk_v, lk_v, hk_v, tv_v, lv_v, hv_v, tm_v, lm_v, hm_v, n1_v, n2_v,
    tm_s, hm_s, turn,
    load_sem, send_sem, arrive_sem, sib_sem, pair_sem, norm_sem,
):
    sh = lax.axis_index("shard")
    tp = lax.axis_index("tp")
    core = lax.rem(sh, 2)
    x = lax.rem(sh // 2, 4)
    z = (sh // 8) * 2 + tp // 4
    y = lax.rem(tp, 4)

    def device(dx=0, dz=0, dy=0, other=False):
        zz = lax.rem(z + dz, 4)
        cc = 1 - core if other else core
        return (
            ((zz // 2) * 4 + lax.rem(x + dx, 4)) * 2 + cc,
            lax.rem(zz, 2) * 4 + lax.rem(y + dy, 4),
        )

    target = {
        "x+": device(dx=1), "x-": device(dx=3), "z": device(dz=2), "d": device(other=True),
    }

    beside = device(dz=1 + 2 * lax.rem(z, 2))
    partners = [device(dx=k) for k in (1, 2, 3)] + [beside, target["z"]]
    partners += [device(dy=k) for k in (1, 3)] + [target["d"]]
    barrier = pltpu.get_barrier_semaphore()
    for partner in partners:
        pl.semaphore_signal(barrier, inc=1, device_id=partner, device_id_type=MESH)

    loads = []
    for k, (src, dst) in enumerate((
        (tq, tq_v), (lq, lq_v), (hq, hq_v), (tm, tm_v), (hm, hm_v), (lm, lm_v), (tk, tk_v), (lk, lk_v), (hk, hk_v),
        (tv, tv_v), (lv, lv_v), (hv, hv_v), (n1, n1_v), (n2, n2_v),
    )):
        copy = pltpu.make_async_copy(src, dst, load_sem.at[k])
        copy.start()
        loads.append(copy)

    def send(src, dst, sent, sem, to):
        copy = pltpu.make_async_remote_copy(
            src_ref=src, dst_ref=dst, send_sem=sent, recv_sem=sem, device_id=to, device_id_type=MESH,
        )
        copy.start()
        return copy

    def waiting(ref, sent, sem):
        return pltpu.make_async_remote_copy(
            src_ref=ref, dst_ref=ref, send_sem=sent, recv_sem=sem, device_id=target["d"], device_id_type=MESH,
        )

    def arrived(dst, sem):
        waiting(dst, send_sem.at[0], sem).wait_recv()

    n_sent = [[0, 0] for _ in range(4)]

    def many(kind, count):
        if kind == 0:
            return q_all.at[pl.ds(0, Q_ROWS * count)]
        if kind < 3:
            return (k_all if kind == 1 else v_all).at[pl.ds(0, 320 * count)]
        if count % 4 == 0:
            return m_all.at[pl.ds(0, count // 4)]
        return m_all.at[pl.ds(0, count // 2), pl.ds(0, 512)]

    def place(chip, cc, chunk):
        row = (chip * 2 + cc) * 320
        if KIND[chunk] in (1, 2):
            return (k_all if KIND[chunk] == 1 else v_all).at[pl.ds(pl.multiple_of(row, 64), 320)]
        if KIND[chunk] == 0:
            return q_all.at[pl.ds(pl.multiple_of(row + Q_ROWS * FROM[chunk], 32), Q_ROWS * WEIGHT[chunk])]
        return m_all.at[
            chip, pl.ds(pl.multiple_of(512 * cc + int(M_ROWS * FROM[chunk]), 64), int(M_ROWS * WEIGHT[chunk]))
        ]

    def chip_at(dz2, dx):
        return (lax.rem(sh // 8 + dz2, 2)) * 4 + lax.rem(x + dx, 4)

    def arrive_index(dz, dx, chunk):
        return SLOTS[(dz, dx, chunk)]

    def dispatch(link, item, src, chip):
        kind, chunk = KIND[item[-1]], item[-1]
        if link == "d":
            sem, side = sib_sem.at[kind], 1
        else:
            dz, dx = (1, item[1]) if link == "z" else (item[1], item[2])
            sem, side = arrive_sem.at[arrive_index(dz, dx, chunk)], 0
        n_sent[kind][side] += WEIGHT[chunk]
        send(src, src, send_sem.at[kind * 2 + side], sem, target[link])

    first, second, third, order = plan()
    own = chip_at(0, 0)

    def wait_loads(*which):
        for k in which:
            loads[k].wait()

    def product(low_turned, high):
        return mix_rate * lax.dot_general(
            low_turned, high, (((0,), (0,)), ((), ())), preferred_element_type=jnp.float32
        )

    row = sh * 320
    wait_loads(12, 13)
    plane = core * 4 + y
    n_all[plane, z, x] = jnp.zeros((1, 128), jnp.float32)
    n_all[plane, z, x, :, 0:40] = n1_v[...] + n2_v[...]
    wait_loads(0, 1, 2)
    q_all[pl.ds(pl.multiple_of(row, 64), 320)] = (
        tq_v[...].astype(jnp.float32) + product(lq_v[...], hq_v[...])
    ).astype(jnp.bfloat16)
    pl.semaphore_wait(barrier, len(partners))
    line = n_all.at[plane, z, x]
    small = [send(line, line, norm_sem.at[8 + k], norm_sem.at[k - 1], device(dx=k)) for k in (1, 2, 3)]
    for link, item in first:
        dispatch(link, item, place(own, core, item[-1]), own)

    half = pl.ds(pl.multiple_of(512 * core, 512), 512)
    other_half = pl.ds(pl.multiple_of(512 * (1 - core), 512), 512)
    wait_loads(3, 4)
    small += [
        send(tm_v.at[:, other_half], tm_s, pair_sem.at[2], pair_sem.at[0], target["d"]),
        send(hm_v, hm_s, pair_sem.at[3], pair_sem.at[1], target["d"]),
    ]

    wait_loads(6, 7, 8, 9, 10, 11)
    k_all[pl.ds(pl.multiple_of(row, 64), 320)] = (
        tk_v[...].astype(jnp.float32) + product(lk_v[...], hk_v[...])
    ).astype(jnp.bfloat16)
    v_all[pl.ds(pl.multiple_of(row, 64), 320)] = (
        tv_v[...].astype(jnp.float32) + product(lv_v[...], hv_v[...])
    ).astype(jnp.bfloat16)
    for link, item in second:
        dispatch(link, item, place(own, core, item[-1]), own)

    wait_loads(5)
    arrived(tm_s, pair_sem.at[0])
    arrived(hm_s, pair_sem.at[1])
    mine = pl.ds(pl.multiple_of(320 * core, 64), 320)
    others = pl.ds(pl.multiple_of(320 * (1 - core), 64), 320)
    low_half = lm_v[:, half]
    own_half = tm_v[:, half]
    for b in range(4):
        cols = slice(128 * b, 128 * (b + 1))
        low = low_half[:, cols]
        turn[b, mine] = own_half[:, cols].astype(jnp.float32) + product(hm_v[...], low)
        turn[b, others] = tm_s[:, cols].astype(jnp.float32) + product(hm_s[...], low)
        rows = pl.ds(pl.multiple_of(512 * core + 128 * b, 128), 128)
        m_all[own, rows] = turn[b].T.astype(jnp.bfloat16)
    for link, item in third:
        dispatch(link, item, place(own, core, item[-1]), own)

    for event in order:
        kind, chunk = event[0], event[-1]
        if kind == "n0":
            for k in (1, 2, 3):
                arrived(n_all.at[plane, z, lax.rem(x + 4 - k, 4)], norm_sem.at[k - 1])
            line = n_all.at[plane, z]
            small.append(send(line, line, norm_sem.at[12], norm_sem.at[3], beside))
        elif kind == "n1":
            arrived(n_all.at[plane, lax.rem(z + 1 + 2 * lax.rem(z, 2), 4)], norm_sem.at[3])
            line = n_all.at[plane, pl.ds((z // 2) * 2, 2)]
            small.append(send(line, line, norm_sem.at[13], norm_sem.at[4], target["z"]))
        elif kind == "n2":
            arrived(n_all.at[plane, pl.ds((1 - z // 2) * 2, 2)], norm_sem.at[4])
            line = n_all.at[plane]
            for k in (1, 3):
                small.append(send(line, line, norm_sem.at[13 + k], norm_sem.at[4 + k], device(dy=k)))
        elif kind == "n3":
            for k in (1, 3):
                arrived(n_all.at[core * 4 + lax.rem(y + 4 - k, 4)], norm_sem.at[4 + k])
            line = n_all.at[core * 4 + lax.rem(y + 3, 4)]
            small.append(send(line, line, norm_sem.at[15], norm_sem.at[6], device(dy=1)))
        elif kind == "n4":
            arrived(n_all.at[core * 4 + lax.rem(y + 2, 4)], norm_sem.at[6])
            line = n_all.at[pl.ds(core * 4, 4)]
            small.append(send(line, line, norm_sem.at[17], norm_sem.at[8], target["d"]))
        elif kind == "n5":
            arrived(n_all.at[pl.ds((1 - core) * 4, 4)], norm_sem.at[8])
            for copy in small:
                copy.wait_send()
        else:
            dz, dx = (1, event[1]) if kind == "z" else (event[1], event[2])
            chip = chip_at(dz, dx)
            src = place(chip, core, chunk)
            arrived(src, arrive_sem.at[arrive_index(dz, dx, chunk)])
            for link, item in react(event):
                at = chip_at(1, 0) if dz == 0 and item[0] == kind and item[1] == 1 else chip
                dispatch(link, item, place(at, core, item[-1]), at)

    for kind, per_piece in enumerate((2, 1, 1, 2)):
        for side in (0, 1):
            count = int(n_sent[kind][side])
            waiting(many(kind, count), send_sem.at[kind * 2 + side], sib_sem.at[0]).wait_send()
        arrived(many(kind, per_piece * 8), sib_sem.at[kind])


def write_kernel(q_all, k_all, v_all, m_all, n_all, q_out, k_out, v_out, m_out, n_out, lines, rounded, sems):
    copies = []
    for k in range(8):
        copies.append((m_all.at[k], m_out.at[:, pl.ds(640 * k, 640)]))
        copies.append((q_all.at[pl.ds(640 * k, 640)], q_out.at[pl.ds(640 * k, 640)]))
    copies += [(k_all, k_out), (v_all, v_out)]
    copies = [pltpu.make_async_copy(src, dst, sems.at[k]) for k, (src, dst) in enumerate(copies)]
    for copy in copies:
        copy.start()
    lane = lax.broadcasted_iota(jnp.int32, (8, 128), 1)
    acc = [jnp.zeros((8, 128), jnp.float32) for _ in range(5)]
    for i in range(16):
        core, zl, y = i // 8, (i // 4) % 2, i % 4
        rows = [n_all[core * 4 + y, zh * 2 + zl, xx] for zh in range(2) for xx in range(4)]
        block = jnp.concatenate(rows, axis=0)
        q, off = (40 * i) // 128, (40 * i) % 128
        turned = pltpu.roll(block, off, 1) if off else block
        acc[q] = jnp.where((lane >= off) & (lane < off + 40), turned, acc[q])
        if off + 40 > 128:
            acc[q + 1] = jnp.where(lane < off + 40 - 128, turned, acc[q + 1])
    for q in range(5):
        lines[pl.ds(q, 8, stride=5), :] = acc[q]
    rounded[...] = lines[...].astype(jnp.bfloat16)
    last = pltpu.make_async_copy(rounded, n_out, sems.at[len(copies)])
    last.start()
    copies.append(last)
    for copy in copies:
        copy.wait()


def body(
    train_query, low_query, high_query, train_key, low_key, high_key, train_value, low_value, high_value,
    train_mixed, low_mixed, high_mixed, norm_train, norm_step,
):
    bf16, f32 = jnp.bfloat16, jnp.float32
    args = (
        train_query, low_query.T, high_query, train_key, low_key.T, high_key, train_value, low_value.T, high_value,
        train_mixed.T, low_mixed.T, high_mixed, norm_train.reshape(1, -1), norm_step.reshape(1, -1),
    )
    vmem = pltpu.MemorySpace.VMEM
    q_all, k_all, v_all, m_all, n_all = pl.pallas_call(
        gather_kernel,
        name="gather",
        out_shape=[
            vmem((5120, 1024), bf16), vmem((5120, 128), bf16), vmem((5120, 128), bf16),
            vmem((8, 1024, 640), bf16), vmem((8, 4, 4, 1, 128), f32),
        ],
        in_specs=[pl.BlockSpec(memory_space=pltpu.MemorySpace.HBM)] * 14,
        out_specs=[pl.BlockSpec(memory_space=vmem)] * 5,
        scratch_shapes=[pltpu.VMEM(a.shape, a.dtype) for a in args] + [
            pltpu.VMEM((320, 512), bf16), pltpu.VMEM((32, 320), bf16), pltpu.VMEM((4, 640, 128), f32),
            pltpu.SemaphoreType.DMA((N_LOADS,)), pltpu.SemaphoreType.DMA((8,)),
            pltpu.SemaphoreType.DMA((len(SLOTS),)), pltpu.SemaphoreType.DMA((4,)),
            pltpu.SemaphoreType.DMA((4,)), pltpu.SemaphoreType.DMA((18,)),
        ],
        compiler_params=pltpu.CompilerParams(
            collective_id=0, has_side_effects=True, vmem_limit_bytes=36 * 1024 * 1024
        ),
    )(*args)
    hbm = pltpu.MemorySpace.HBM
    q, k, v, m, n = pl.pallas_call(
        write_kernel,
        name="write",
        out_shape=[
            jax.ShapeDtypeStruct((5120, 1024), bf16), jax.ShapeDtypeStruct((5120, 128), bf16),
            jax.ShapeDtypeStruct((5120, 128), bf16), jax.ShapeDtypeStruct((1024, 5120), bf16),
            jax.ShapeDtypeStruct((40, 128), bf16),
        ],
        in_specs=[pl.BlockSpec(memory_space=vmem)] * 5,
        out_specs=[pl.BlockSpec(memory_space=hbm)] * 5,
        scratch_shapes=[pltpu.VMEM((40, 128), f32), pltpu.VMEM((40, 128), bf16), pltpu.SemaphoreType.DMA((19,))],
        compiler_params=pltpu.CompilerParams(vmem_limit_bytes=2 * 1024 * 1024),
    )(q_all, k_all, v_all, m_all, n_all)
    return q, k, v, m, n.reshape(5120)


def solution(mesh):
    return jax.shard_map(
        body,
        mesh=mesh,
        in_specs=(
            P("shard", "tp"), P("shard", None), P(None, "tp"),
            P("shard", "tp"), P("shard", None), P(None, "tp"),
            P("shard", "tp"), P("shard", None), P(None, "tp"),
            P("tp", "shard"), P("tp", None), P(None, "shard"),
            P(("shard", "tp")), P(("shard", "tp")),
        ),
        out_specs=(P(None, "tp"), P(None, "tp"), P(None, "tp"), P("tp", None), P()),
        check_vma=False,
    )
```

```python
import functools
import heapq

import jax
import jax.numpy as jnp
from jax import lax
from jax.experimental import pallas as pl
from jax.experimental.pallas import tpu as pltpu
from jax.sharding import PartitionSpec as P

MESH = pl.DeviceIdType.MESH
mix_rate = 0.5

Q_ROWS = 160
M_ROWS = 256
KIND = (0, 1, 0, 2, 3, 3, 0, 3, 3, 3)
FROM = (0, 0, 1, 0, 0, 1, 0, 0, 1, 1.75)
WEIGHT = (1, 1, 1, 1, 1, 1, 2, 2, 0.75, 0.25)
SIZES = (327680, 81920, 327680, 81920, 327680, 327680, 655360, 655360, 245760, 81920)
ONWARD = {"x+": {6: 0, 0: 0, 1: 1, 7: 4}, "x-": {6: 2, 2: 2, 3: 3, 7: 5}}
PARTNERS = {"x+": (0, 1, 2, 3), "x-": (2, 3, 0, 1)}


def own_sends(chunk, along_x, along_z):
    sends = []
    if along_z:
        sends.append(("z", ("z", 0, chunk)))
    if along_x:
        sends += [("x+", ("x+", 0, 3, chunk)), ("x-", ("x-", 0, 1, chunk))]
    if along_z:
        sends.append(("d", ("d", 0, 0, chunk)))
    return sends


def react(event):
    kind = event[0]
    if kind == "z":
        _, dx, chunk = event
        return [("d", ("d", 1, dx, chunk))]
    _, dz, dx, chunk = event
    sends = []
    if dx != 2 and chunk in ONWARD[kind]:
        sends.append((kind, (kind, dz, 2, ONWARD[kind][chunk])))
        if (dz, chunk) == (0, 7):
            sends += [(kind, (kind, 1, dx, other)) for other in PARTNERS[kind]]
    if KIND[chunk] == 3 and dz == 0:
        sends += [("z", ("z", dx, part)) for part in ((8, 9) if chunk == 5 else (chunk,))]
    sends.append(("d", ("d", dz, dx, chunk)))
    return sends


def plan():
    first = []
    for chunk in (6,):
        first += own_sends(chunk, True, True)
    second = []
    for chunk in (1, 3):
        second += own_sends(chunk, False, True)
    third = []
    for chunk in (7,):
        third += own_sends(chunk, True, True)
    for chunk in (1, 3):
        third += own_sends(chunk, True, False)
    starts = [(2.0, first), (2.2, second), (5.5, third)]
    heap, count, free, order = [], 0, {}, []
    for time, sends in starts:
        heapq.heappush(heap, (time, count, None, sends))
        count += 1
    while heap:
        time, _, event, sends = heapq.heappop(heap)
        if event is not None:
            order.append((time, event))
            sends = react(event)
        for link, item in sends:
            if link == "d":
                continue
            done = max(time, free.get(link, 0.0)) + SIZES[item[-1]] / 45000.0
            free[link] = done
            heapq.heappush(heap, (done + 1.9, count, item, None))
            count += 1
    order += [(t, (name,)) for t, name in ((30.0, "n1"), (42.0, "n2"), (45.0, "n3"), (48.0, "n4"), (51.0, "n5"), (60.0, "n6"))]
    order = [event for _, event in sorted(order, key=lambda pair: pair[0])]
    held = [order.index(("x+", 0, 3, 7)), order.index(("x-", 0, 1, 7))]
    assert min(held) > max(order.index(("z", 0, chunk)) for chunk in (6, 1, 3))
    return first, second, third, order


def slots():
    found = {}
    for event in plan()[3]:
        if event[0][0] != "n":
            dz, dx = (1, event[1]) if event[0] == "z" else (event[1], event[2])
            found[(dz, dx, event[-1])] = len(found)
    return found


SLOTS = slots()
N_LOADS = 14


def gather_kernel(
    tq, lq, hq, tk, lk, hk, tv, lv, hv, tm, lm, hm, n1, n2,
    q_all, k_all, v_all, m_all, n_all,
    tq_v, lq_v, hq_v, tk_v, lk_v, hk_v, tv_v, lv_v, hv_v, tm_v, lm_v, hm_v, n1_v, n2_v,
    tm_s, hm_s, turn,
    load_sem, send_sem, arrive_sem, sib_sem, pair_sem, norm_sem,
):
    sh = lax.axis_index("shard")
    tp = lax.axis_index("tp")
    core = lax.rem(sh, 2)
    x = lax.rem(sh // 2, 4)
    z = (sh // 8) * 2 + tp // 4
    y = lax.rem(tp, 4)

    def device(dx=0, dz=0, dy=0, other=False):
        zz = lax.rem(z + dz, 4)
        cc = 1 - core if other else core
        return (
            ((zz // 2) * 4 + lax.rem(x + dx, 4)) * 2 + cc,
            lax.rem(zz, 2) * 4 + lax.rem(y + dy, 4),
        )

    target = {
        "x+": device(dx=1), "x-": device(dx=3), "z": device(dz=2), "d": device(other=True),
    }

    beside = device(dz=1 + 2 * lax.rem(z, 2))
    pair = device(dy=1 + 2 * lax.rem(y, 2))
    inner = lax.rem((y + 1) // 2, 2)
    across = device(dy=7 - 2 * y)
    partners = [device(dx=k) for k in (1, 2, 3)] + [beside, target["z"], pair, target["d"]]
    barrier = pltpu.get_barrier_semaphore()
    for partner in partners:
        pl.semaphore_signal(barrier, inc=1, device_id=partner, device_id_type=MESH)

    @pl.when(inner == 1)
    def _():
        pl.semaphore_signal(barrier, inc=1, device_id=across, device_id_type=MESH)


    loads = []
    for k, (src, dst) in enumerate((
        (tq, tq_v), (lq, lq_v), (hq, hq_v), (tm, tm_v), (hm, hm_v), (lm, lm_v), (tk, tk_v), (lk, lk_v), (hk, hk_v),
        (tv, tv_v), (lv, lv_v), (hv, hv_v), (n1, n1_v), (n2, n2_v),
    )):
        copy = pltpu.make_async_copy(src, dst, load_sem.at[k])
        copy.start()
        loads.append(copy)

    def send(src, dst, sent, sem, to):
        copy = pltpu.make_async_remote_copy(
            src_ref=src, dst_ref=dst, send_sem=sent, recv_sem=sem, device_id=to, device_id_type=MESH,
        )
        copy.start()
        return copy

    def waiting(ref, sent, sem):
        return pltpu.make_async_remote_copy(
            src_ref=ref, dst_ref=ref, send_sem=sent, recv_sem=sem, device_id=target["d"], device_id_type=MESH,
        )

    def arrived(dst, sem):
        waiting(dst, send_sem.at[0], sem).wait_recv()

    n_sent = [[0, 0] for _ in range(4)]

    def many(kind, count):
        if kind == 0:
            return q_all.at[pl.ds(0, Q_ROWS * count)]
        if kind < 3:
            return (k_all if kind == 1 else v_all).at[pl.ds(0, 320 * count)]
        if count % 4 == 0:
            return m_all.at[pl.ds(0, count // 4)]
        return m_all.at[pl.ds(0, count // 2), pl.ds(0, 512)]

    def place(chip, cc, chunk):
        row = (chip * 2 + cc) * 320
        if KIND[chunk] in (1, 2):
            return (k_all if KIND[chunk] == 1 else v_all).at[pl.ds(pl.multiple_of(row, 64), 320)]
        if KIND[chunk] == 0:
            return q_all.at[pl.ds(pl.multiple_of(row + Q_ROWS * FROM[chunk], 32), Q_ROWS * WEIGHT[chunk])]
        return m_all.at[
            chip, pl.ds(pl.multiple_of(512 * cc + int(M_ROWS * FROM[chunk]), 64), int(M_ROWS * WEIGHT[chunk]))
        ]

    def chip_at(dz2, dx):
        return (lax.rem(sh // 8 + dz2, 2)) * 4 + lax.rem(x + dx, 4)

    def arrive_index(dz, dx, chunk):
        return SLOTS[(dz, dx, chunk)]

    def dispatch(link, item, src, chip):
        kind, chunk = KIND[item[-1]], item[-1]
        if link == "d":
            sem, side = sib_sem.at[kind], 1
        else:
            dz, dx = (1, item[1]) if link == "z" else (item[1], item[2])
            sem, side = arrive_sem.at[arrive_index(dz, dx, chunk)], 0
        n_sent[kind][side] += WEIGHT[chunk]
        send(src, src, send_sem.at[kind * 2 + side], sem, target[link])

    first, second, third, order = plan()
    own = chip_at(0, 0)

    def wait_loads(*which):
        for k in which:
            loads[k].wait()

    def product(low_turned, high):
        return mix_rate * lax.dot_general(
            low_turned, high, (((0,), (0,)), ((), ())), preferred_element_type=jnp.float32
        )

    row = sh * 320
    wait_loads(12, 13)
    plane = core * 4 + y
    n_all[plane, z, x] = jnp.zeros((1, 128), jnp.float32)
    n_all[plane, z, x, :, 0:40] = n1_v[...] + n2_v[...]
    wait_loads(0, 1, 2)
    q_all[pl.ds(pl.multiple_of(row, 64), 320)] = (
        tq_v[...].astype(jnp.float32) + product(lq_v[...], hq_v[...])
    ).astype(jnp.bfloat16)
    pl.semaphore_wait(barrier, len(partners) + inner)
    line = n_all.at[plane, z, x]
    small = [send(line, line, norm_sem.at[8 + k], norm_sem.at[k - 1], device(dx=k)) for k in (1, 2, 3)]
    for link, item in first:
        dispatch(link, item, place(own, core, item[-1]), own)

    half = pl.ds(pl.multiple_of(512 * core, 512), 512)
    other_half = pl.ds(pl.multiple_of(512 * (1 - core), 512), 512)
    wait_loads(3, 4)
    small += [
        send(tm_v.at[:, other_half], tm_s, pair_sem.at[2], pair_sem.at[0], target["d"]),
        send(hm_v, hm_s, pair_sem.at[3], pair_sem.at[1], target["d"]),
    ]

    wait_loads(6, 7, 8, 9, 10, 11)
    k_all[pl.ds(pl.multiple_of(row, 64), 320)] = (
        tk_v[...].astype(jnp.float32) + product(lk_v[...], hk_v[...])
    ).astype(jnp.bfloat16)
    v_all[pl.ds(pl.multiple_of(row, 64), 320)] = (
        tv_v[...].astype(jnp.float32) + product(lv_v[...], hv_v[...])
    ).astype(jnp.bfloat16)
    for link, item in second:
        dispatch(link, item, place(own, core, item[-1]), own)

    wait_loads(5)
    arrived(tm_s, pair_sem.at[0])
    arrived(hm_s, pair_sem.at[1])
    mine = pl.ds(pl.multiple_of(320 * core, 64), 320)
    others = pl.ds(pl.multiple_of(320 * (1 - core), 64), 320)
    low_half = lm_v[:, half]
    own_half = tm_v[:, half]
    for b in range(4):
        cols = slice(128 * b, 128 * (b + 1))
        low = low_half[:, cols]
        turn[b, mine] = own_half[:, cols].astype(jnp.float32) + product(hm_v[...], low)
        turn[b, others] = tm_s[:, cols].astype(jnp.float32) + product(hm_s[...], low)
        rows = pl.ds(pl.multiple_of(512 * core + 128 * b, 128), 128)
        m_all[own, rows] = turn[b].T.astype(jnp.bfloat16)
    for k in (1, 2, 3):
        arrived(n_all.at[plane, z, lax.rem(x + 4 - k, 4)], norm_sem.at[k - 1])
    line = n_all.at[plane, z]
    small.append(send(line, line, norm_sem.at[12], norm_sem.at[3], beside))
    for link, item in third:
        dispatch(link, item, place(own, core, item[-1]), own)

    for event in order:
        kind, chunk = event[0], event[-1]
        if kind == "n1":
            arrived(n_all.at[plane, lax.rem(z + 1 + 2 * lax.rem(z, 2), 4)], norm_sem.at[3])
            line = n_all.at[plane, pl.ds((z // 2) * 2, 2)]
            small.append(send(line, line, norm_sem.at[13], norm_sem.at[4], target["z"]))
        elif kind == "n2":
            arrived(n_all.at[plane, pl.ds((1 - z // 2) * 2, 2)], norm_sem.at[4])
            line = n_all.at[plane]
            small.append(send(line, line, norm_sem.at[14], norm_sem.at[5], pair))
        elif kind == "n3":
            arrived(n_all.at[core * 4 + y + 1 - 2 * lax.rem(y, 2)], norm_sem.at[5])
            near = n_all.at[pl.ds(core * 4 + (y // 2) * 2, 2)]
            far = n_all.at[pl.ds(core * 4 + (1 - y // 2) * 2, 2)]

            @pl.when(inner == 1)
            def _():
                send(near, near, norm_sem.at[15], norm_sem.at[6], across)
        elif kind == "n4":

            @pl.when(inner == 1)
            def _():
                arrived(far, norm_sem.at[6])
                send(far, far, norm_sem.at[16], norm_sem.at[7], pair)
        elif kind == "n5":

            @pl.when(inner == 0)
            def _():
                arrived(far, norm_sem.at[7])

            line = n_all.at[pl.ds(core * 4, 4)]
            small.append(send(line, line, norm_sem.at[17], norm_sem.at[8], target["d"]))
        elif kind == "n6":
            arrived(n_all.at[pl.ds((1 - core) * 4, 4)], norm_sem.at[8])

            @pl.when(inner == 1)
            def _():
                waiting(near, norm_sem.at[15], norm_sem.at[6]).wait_send()
                waiting(far, norm_sem.at[16], norm_sem.at[7]).wait_send()

            for copy in small:
                copy.wait_send()
        else:
            dz, dx = (1, event[1]) if kind == "z" else (event[1], event[2])
            chip = chip_at(dz, dx)
            src = place(chip, core, chunk)
            arrived(src, arrive_sem.at[arrive_index(dz, dx, chunk)])
            for link, item in react(event):
                at = chip_at(1, 0) if dz == 0 and item[0] == kind and item[1] == 1 else chip
                dispatch(link, item, place(at, core, item[-1]), at)

    for kind, per_piece in enumerate((2, 1, 1, 2)):
        for side in (0, 1):
            count = int(n_sent[kind][side])
            waiting(many(kind, count), send_sem.at[kind * 2 + side], sib_sem.at[0]).wait_send()
        arrived(many(kind, per_piece * 8), sib_sem.at[kind])


def write_kernel(q_all, k_all, v_all, m_all, n_all, q_out, k_out, v_out, m_out, n_out, lines, rounded, sems):
    copies = []
    for k in range(8):
        copies.append((m_all.at[k], m_out.at[:, pl.ds(640 * k, 640)]))
        copies.append((q_all.at[pl.ds(640 * k, 640)], q_out.at[pl.ds(640 * k, 640)]))
    copies += [(k_all, k_out), (v_all, v_out)]
    copies = [pltpu.make_async_copy(src, dst, sems.at[k]) for k, (src, dst) in enumerate(copies)]
    for copy in copies:
        copy.start()
    lane = lax.broadcasted_iota(jnp.int32, (8, 128), 1)
    acc = [jnp.zeros((8, 128), jnp.float32) for _ in range(5)]
    for i in range(16):
        core, zl, y = i // 8, (i // 4) % 2, i % 4
        rows = [n_all[core * 4 + y, zh * 2 + zl, xx] for zh in range(2) for xx in range(4)]
        block = jnp.concatenate(rows, axis=0)
        q, off = (40 * i) // 128, (40 * i) % 128
        turned = pltpu.roll(block, off, 1) if off else block
        acc[q] = jnp.where((lane >= off) & (lane < off + 40), turned, acc[q])
        if off + 40 > 128:
            acc[q + 1] = jnp.where(lane < off + 40 - 128, turned, acc[q + 1])
    for q in range(5):
        lines[pl.ds(q, 8, stride=5), :] = acc[q]
    rounded[...] = lines[...].astype(jnp.bfloat16)
    last = pltpu.make_async_copy(rounded, n_out, sems.at[len(copies)])
    last.start()
    copies.append(last)
    for copy in copies:
        copy.wait()


def body(
    train_query, low_query, high_query, train_key, low_key, high_key, train_value, low_value, high_value,
    train_mixed, low_mixed, high_mixed, norm_train, norm_step,
):
    bf16, f32 = jnp.bfloat16, jnp.float32
    args = (
        train_query, low_query.T, high_query, train_key, low_key.T, high_key, train_value, low_value.T, high_value,
        train_mixed.T, low_mixed.T, high_mixed, norm_train.reshape(1, -1), norm_step.reshape(1, -1),
    )
    vmem = pltpu.MemorySpace.VMEM
    q_all, k_all, v_all, m_all, n_all = pl.pallas_call(
        gather_kernel,
        name="gather",
        out_shape=[
            vmem((5120, 1024), bf16), vmem((5120, 128), bf16), vmem((5120, 128), bf16),
            vmem((8, 1024, 640), bf16), vmem((8, 4, 4, 1, 128), f32),
        ],
        in_specs=[pl.BlockSpec(memory_space=pltpu.MemorySpace.HBM)] * 14,
        out_specs=[pl.BlockSpec(memory_space=vmem)] * 5,
        scratch_shapes=[pltpu.VMEM(a.shape, a.dtype) for a in args] + [
            pltpu.VMEM((320, 512), bf16), pltpu.VMEM((32, 320), bf16), pltpu.VMEM((4, 640, 128), f32),
            pltpu.SemaphoreType.DMA((N_LOADS,)), pltpu.SemaphoreType.DMA((8,)),
            pltpu.SemaphoreType.DMA((len(SLOTS),)), pltpu.SemaphoreType.DMA((4,)),
            pltpu.SemaphoreType.DMA((4,)), pltpu.SemaphoreType.DMA((18,)),
        ],
        compiler_params=pltpu.CompilerParams(
            collective_id=0, has_side_effects=True, vmem_limit_bytes=36 * 1024 * 1024
        ),
    )(*args)
    hbm = pltpu.MemorySpace.HBM
    q, k, v, m, n = pl.pallas_call(
        write_kernel,
        name="write",
        out_shape=[
            jax.ShapeDtypeStruct((5120, 1024), bf16), jax.ShapeDtypeStruct((5120, 128), bf16),
            jax.ShapeDtypeStruct((5120, 128), bf16), jax.ShapeDtypeStruct((1024, 5120), bf16),
            jax.ShapeDtypeStruct((40, 128), bf16),
        ],
        in_specs=[pl.BlockSpec(memory_space=vmem)] * 5,
        out_specs=[pl.BlockSpec(memory_space=hbm)] * 5,
        scratch_shapes=[pltpu.VMEM((40, 128), f32), pltpu.VMEM((40, 128), bf16), pltpu.SemaphoreType.DMA((19,))],
        compiler_params=pltpu.CompilerParams(vmem_limit_bytes=2 * 1024 * 1024),
    )(q_all, k_all, v_all, m_all, n_all)
    return q, k, v, m, n.reshape(5120)


def solution(mesh):
    return jax.shard_map(
        body,
        mesh=mesh,
        in_specs=(
            P("shard", "tp"), P("shard", None), P(None, "tp"),
            P("shard", "tp"), P("shard", None), P(None, "tp"),
            P("shard", "tp"), P("shard", None), P(None, "tp"),
            P("tp", "shard"), P("tp", None), P(None, "shard"),
            P(("shard", "tp")), P(("shard", "tp")),
        ),
        out_specs=(P(None, "tp"), P(None, "tp"), P(None, "tp"), P("tp", None), P()),
        check_vma=False,
    )
```

```python
import functools
import heapq

import jax
import jax.numpy as jnp
from jax import lax
from jax.experimental import pallas as pl
from jax.experimental.pallas import tpu as pltpu
from jax.sharding import PartitionSpec as P

MESH = pl.DeviceIdType.MESH
mix_rate = 0.5

Q_ROWS = 160
M_ROWS = 256
KIND = (0, 1, 0, 2, 3, 3, 0, 3, 3, 3)
FROM = (0, 0, 1, 0, 0, 1, 0, 0, 1, 1.75)
WEIGHT = (1, 1, 1, 1, 1, 1, 2, 2, 0.75, 0.25)
SIZES = (327680, 81920, 327680, 81920, 327680, 327680, 655360, 655360, 245760, 81920)
ONWARD = {"x+": {6: 0, 0: 0, 1: 1, 7: 4}, "x-": {6: 2, 2: 2, 3: 3, 7: 5}}
PARTNERS = {"x+": (0, 1, 2, 3), "x-": (2, 3, 0, 1)}


def own_sends(chunk, along_x, along_z):
    sends = []
    if along_z:
        sends.append(("z", ("z", 0, chunk)))
    if along_x:
        sends += [("x+", ("x+", 0, 3, chunk)), ("x-", ("x-", 0, 1, chunk))]
    if along_z:
        sends.append(("d", ("d", 0, 0, chunk)))
    return sends


def react(event):
    kind = event[0]
    if kind == "z":
        _, dx, chunk = event
        return [("d", ("d", 1, dx, chunk))]
    _, dz, dx, chunk = event
    sends = []
    if dx != 2 and chunk in ONWARD[kind]:
        sends.append((kind, (kind, dz, 2, ONWARD[kind][chunk])))
        if (dz, chunk) == (0, 7):
            sends += [(kind, (kind, 1, dx, other)) for other in PARTNERS[kind]]
    if KIND[chunk] == 3 and dz == 0:
        sends += [("z", ("z", dx, part)) for part in ((8, 9) if chunk == 5 else (chunk,))]
    sends.append(("d", ("d", dz, dx, chunk)))
    return sends


def plan():
    first = []
    for chunk in (6,):
        first += own_sends(chunk, True, True)
    second = []
    for chunk in (1, 3):
        second += own_sends(chunk, False, True)
    third = []
    for chunk in (7,):
        third += own_sends(chunk, True, True)
    for chunk in (1, 3):
        third += own_sends(chunk, True, False)
    starts = [(2.0, first), (2.2, second), (5.5, third)]
    heap, count, free, order = [], 0, {}, []
    for time, sends in starts:
        heapq.heappush(heap, (time, count, None, sends))
        count += 1
    while heap:
        time, _, event, sends = heapq.heappop(heap)
        if event is not None:
            order.append((time, event))
            sends = react(event)
        for link, item in sends:
            if link == "d":
                continue
            done = max(time, free.get(link, 0.0)) + SIZES[item[-1]] / 45000.0
            free[link] = done
            heapq.heappush(heap, (done + 1.9, count, item, None))
            count += 1
    order += [(t, (name,)) for t, name in ((30.0, "n1"), (42.0, "n2"), (45.0, "n3"), (48.0, "n4"), (51.0, "n5"), (60.0, "n6"))]
    order = [event for _, event in sorted(order, key=lambda pair: pair[0])]
    held = [order.index(("x+", 0, 3, 7)), order.index(("x-", 0, 1, 7))]
    assert min(held) > max(order.index(("z", 0, chunk)) for chunk in (6, 1, 3))
    return first, second, third, order


def slots():
    found = {}
    for event in plan()[3]:
        if event[0][0] != "n":
            dz, dx = (1, event[1]) if event[0] == "z" else (event[1], event[2])
            found[(dz, dx, event[-1])] = len(found)
    return found


SLOTS = slots()
N_LOADS = 14


def gather_kernel(
    tq, lq, hq, tk, lk, hk, tv, lv, hv, tm, lm, hm, n1, n2,
    q_all, k_all, v_all, m_all, n_all,
    tq_v, lq_v, hq_v, tk_v, lk_v, hk_v, tv_v, lv_v, hv_v, tm_v, lm_v, hm_v, n1_v, n2_v,
    tm_s, hm_s, turn,
    load_sem, send_sem, arrive_sem, sib_sem, pair_sem, norm_sem,
):
    sh = lax.axis_index("shard")
    tp = lax.axis_index("tp")
    core = lax.rem(sh, 2)
    x = lax.rem(sh // 2, 4)
    z = (sh // 8) * 2 + tp // 4
    y = lax.rem(tp, 4)

    def device(dx=0, dz=0, dy=0, other=False):
        zz = lax.rem(z + dz, 4)
        cc = 1 - core if other else core
        return (
            ((zz // 2) * 4 + lax.rem(x + dx, 4)) * 2 + cc,
            lax.rem(zz, 2) * 4 + lax.rem(y + dy, 4),
        )

    target = {
        "x+": device(dx=1), "x-": device(dx=3), "z": device(dz=2), "d": device(other=True),
    }

    loads = [
        pltpu.make_async_copy(src, dst, load_sem.at[k])
        for k, (src, dst) in enumerate((
            (lq, lq_v), (hq, hq_v), (tq, tq_v), (n1, n1_v), (n2, n2_v), (tm, tm_v), (hm, hm_v), (lm, lm_v),
            (tk, tk_v), (lk, lk_v), (hk, hk_v), (tv, tv_v), (lv, lv_v), (hv, hv_v),
        ))
    ]
    for copy in loads[:5]:
        copy.start()

    beside = device(dz=1 + 2 * lax.rem(z, 2))
    pair = device(dy=1 + 2 * lax.rem(y, 2))
    inner = lax.rem((y + 1) // 2, 2)
    across = device(dy=7 - 2 * y)
    partners = [device(dx=k) for k in (1, 2, 3)] + [beside, target["z"], pair, target["d"]]
    barrier = pltpu.get_barrier_semaphore()
    for partner in partners:
        pl.semaphore_signal(barrier, inc=1, device_id=partner, device_id_type=MESH)

    @pl.when(inner == 1)
    def _():
        pl.semaphore_signal(barrier, inc=1, device_id=across, device_id_type=MESH)


    for copy in loads[5:]:
        copy.start()

    def send(src, dst, sent, sem, to):
        copy = pltpu.make_async_remote_copy(
            src_ref=src, dst_ref=dst, send_sem=sent, recv_sem=sem, device_id=to, device_id_type=MESH,
        )
        copy.start()
        return copy

    def waiting(ref, sent, sem):
        return pltpu.make_async_remote_copy(
            src_ref=ref, dst_ref=ref, send_sem=sent, recv_sem=sem, device_id=target["d"], device_id_type=MESH,
        )

    def arrived(dst, sem):
        waiting(dst, send_sem.at[0], sem).wait_recv()

    n_sent = [[0, 0] for _ in range(4)]

    def many(kind, count):
        if kind == 0:
            return q_all.at[pl.ds(0, Q_ROWS * count)]
        if kind < 3:
            return (k_all if kind == 1 else v_all).at[pl.ds(0, 320 * count)]
        if count % 4 == 0:
            return m_all.at[pl.ds(0, count // 4)]
        return m_all.at[pl.ds(0, count // 2), pl.ds(0, 512)]

    def place(chip, cc, chunk):
        row = (chip * 2 + cc) * 320
        if KIND[chunk] in (1, 2):
            return (k_all if KIND[chunk] == 1 else v_all).at[pl.ds(pl.multiple_of(row, 64), 320)]
        if KIND[chunk] == 0:
            return q_all.at[pl.ds(pl.multiple_of(row + Q_ROWS * FROM[chunk], 32), Q_ROWS * WEIGHT[chunk])]
        return m_all.at[
            chip, pl.ds(pl.multiple_of(512 * cc + int(M_ROWS * FROM[chunk]), 64), int(M_ROWS * WEIGHT[chunk]))
        ]

    def chip_at(dz2, dx):
        return (lax.rem(sh // 8 + dz2, 2)) * 4 + lax.rem(x + dx, 4)

    def arrive_index(dz, dx, chunk):
        return SLOTS[(dz, dx, chunk)]

    def dispatch(link, item, src, chip):
        kind, chunk = KIND[item[-1]], item[-1]
        if link == "d":
            sem, side = sib_sem.at[kind], 1
        else:
            dz, dx = (1, item[1]) if link == "z" else (item[1], item[2])
            sem, side = arrive_sem.at[arrive_index(dz, dx, chunk)], 0
        n_sent[kind][side] += WEIGHT[chunk]
        send(src, src, send_sem.at[kind * 2 + side], sem, target[link])

    first, second, third, order = plan()
    own = chip_at(0, 0)

    def wait_loads(*which):
        for k in which:
            loads[k].wait()

    def product(low_turned, high):
        return mix_rate * lax.dot_general(
            low_turned, high, (((0,), (0,)), ((), ())), preferred_element_type=jnp.float32
        )

    row = sh * 320
    wait_loads(3, 4)
    plane = core * 4 + y
    n_all[plane, z, x] = jnp.zeros((1, 128), jnp.float32)
    n_all[plane, z, x, :, 0:40] = n1_v[...] + n2_v[...]
    wait_loads(0, 1, 2)
    q_all[pl.ds(pl.multiple_of(row, 64), 320)] = (
        tq_v[...].astype(jnp.float32) + product(lq_v[...], hq_v[...])
    ).astype(jnp.bfloat16)
    pl.semaphore_wait(barrier, len(partners) + inner)
    line = n_all.at[plane, z, x]
    small = [send(line, line, norm_sem.at[8 + k], norm_sem.at[k - 1], device(dx=k)) for k in (1, 2, 3)]
    for link, item in first:
        dispatch(link, item, place(own, core, item[-1]), own)

    half = pl.ds(pl.multiple_of(512 * core, 512), 512)
    other_half = pl.ds(pl.multiple_of(512 * (1 - core), 512), 512)
    wait_loads(5, 6)
    small += [
        send(tm_v.at[:, other_half], tm_s, pair_sem.at[2], pair_sem.at[0], target["d"]),
        send(hm_v, hm_s, pair_sem.at[3], pair_sem.at[1], target["d"]),
    ]

    wait_loads(8, 9, 10, 11, 12, 13)
    k_all[pl.ds(pl.multiple_of(row, 64), 320)] = (
        tk_v[...].astype(jnp.float32) + product(lk_v[...], hk_v[...])
    ).astype(jnp.bfloat16)
    v_all[pl.ds(pl.multiple_of(row, 64), 320)] = (
        tv_v[...].astype(jnp.float32) + product(lv_v[...], hv_v[...])
    ).astype(jnp.bfloat16)
    for link, item in second:
        dispatch(link, item, place(own, core, item[-1]), own)

    wait_loads(7)
    arrived(tm_s, pair_sem.at[0])
    arrived(hm_s, pair_sem.at[1])
    mine = pl.ds(pl.multiple_of(320 * core, 64), 320)
    others = pl.ds(pl.multiple_of(320 * (1 - core), 64), 320)
    low_half = lm_v[:, half]
    own_half = tm_v[:, half]
    for b in range(4):
        cols = slice(128 * b, 128 * (b + 1))
        low = low_half[:, cols]
        turn[b, mine] = own_half[:, cols].astype(jnp.float32) + product(hm_v[...], low)
        turn[b, others] = tm_s[:, cols].astype(jnp.float32) + product(hm_s[...], low)
        rows = pl.ds(pl.multiple_of(512 * core + 128 * b, 128), 128)
        m_all[own, rows] = turn[b].T.astype(jnp.bfloat16)
    for k in (1, 2, 3):
        arrived(n_all.at[plane, z, lax.rem(x + 4 - k, 4)], norm_sem.at[k - 1])
    line = n_all.at[plane, z]
    small.append(send(line, line, norm_sem.at[12], norm_sem.at[3], beside))
    for link, item in third:
        dispatch(link, item, place(own, core, item[-1]), own)

    for event in order:
        kind, chunk = event[0], event[-1]
        if kind == "n1":
            arrived(n_all.at[plane, lax.rem(z + 1 + 2 * lax.rem(z, 2), 4)], norm_sem.at[3])
            line = n_all.at[plane, pl.ds((z // 2) * 2, 2)]
            small.append(send(line, line, norm_sem.at[13], norm_sem.at[4], target["z"]))
        elif kind == "n2":
            arrived(n_all.at[plane, pl.ds((1 - z // 2) * 2, 2)], norm_sem.at[4])
            line = n_all.at[plane]
            small.append(send(line, line, norm_sem.at[14], norm_sem.at[5], pair))
        elif kind == "n3":
            arrived(n_all.at[core * 4 + y + 1 - 2 * lax.rem(y, 2)], norm_sem.at[5])
            near = n_all.at[pl.ds(core * 4 + (y // 2) * 2, 2)]
            far = n_all.at[pl.ds(core * 4 + (1 - y // 2) * 2, 2)]

            @pl.when(inner == 1)
            def _():
                send(near, near, norm_sem.at[15], norm_sem.at[6], across)
        elif kind == "n4":

            @pl.when(inner == 1)
            def _():
                arrived(far, norm_sem.at[6])
                send(far, far, norm_sem.at[16], norm_sem.at[7], pair)
        elif kind == "n5":

            @pl.when(inner == 0)
            def _():
                arrived(far, norm_sem.at[7])

            line = n_all.at[pl.ds(core * 4, 4)]
            small.append(send(line, line, norm_sem.at[17], norm_sem.at[8], target["d"]))
        elif kind == "n6":
            arrived(n_all.at[pl.ds((1 - core) * 4, 4)], norm_sem.at[8])

            @pl.when(inner == 1)
            def _():
                waiting(near, norm_sem.at[15], norm_sem.at[6]).wait_send()
                waiting(far, norm_sem.at[16], norm_sem.at[7]).wait_send()

            for copy in small:
                copy.wait_send()
        else:
            dz, dx = (1, event[1]) if kind == "z" else (event[1], event[2])
            chip = chip_at(dz, dx)
            src = place(chip, core, chunk)
            arrived(src, arrive_sem.at[arrive_index(dz, dx, chunk)])
            for link, item in react(event):
                at = chip_at(1, 0) if dz == 0 and item[0] == kind and item[1] == 1 else chip
                dispatch(link, item, place(at, core, item[-1]), at)

    for kind, per_piece in enumerate((2, 1, 1, 2)):
        for side in (0, 1):
            count = int(n_sent[kind][side])
            waiting(many(kind, count), send_sem.at[kind * 2 + side], sib_sem.at[0]).wait_send()
        arrived(many(kind, per_piece * 8), sib_sem.at[kind])


def write_kernel(q_all, k_all, v_all, m_all, n_all, q_out, k_out, v_out, m_out, n_out, lines, rounded, sems):
    copies = []
    for k in range(8):
        copies.append((m_all.at[k], m_out.at[:, pl.ds(640 * k, 640)]))
        if k % 4 == 0:
            copies.append((q_all.at[pl.ds(640 * k, 2560)], q_out.at[pl.ds(640 * k, 2560)]))
    copies += [(k_all, k_out), (v_all, v_out)]
    copies = [pltpu.make_async_copy(src, dst, sems.at[k]) for k, (src, dst) in enumerate(copies)]
    for copy in copies:
        copy.start()
    lane = lax.broadcasted_iota(jnp.int32, (8, 128), 1)
    acc = [jnp.zeros((8, 128), jnp.float32) for _ in range(5)]
    for i in range(16):
        core, zl, y = i // 8, (i // 4) % 2, i % 4
        rows = [n_all[core * 4 + y, zh * 2 + zl, xx] for zh in range(2) for xx in range(4)]
        block = jnp.concatenate(rows, axis=0)
        q, off = (40 * i) // 128, (40 * i) % 128
        turned = pltpu.roll(block, off, 1) if off else block
        acc[q] = jnp.where((lane >= off) & (lane < off + 40), turned, acc[q])
        if off + 40 > 128:
            acc[q + 1] = jnp.where(lane < off + 40 - 128, turned, acc[q + 1])
    for q in range(5):
        lines[pl.ds(q, 8, stride=5), :] = acc[q]
    rounded[...] = lines[...].astype(jnp.bfloat16)
    last = pltpu.make_async_copy(rounded, n_out, sems.at[len(copies)])
    last.start()
    copies.append(last)
    for copy in copies:
        copy.wait()


def body(
    train_query, low_query, high_query, train_key, low_key, high_key, train_value, low_value, high_value,
    train_mixed, low_mixed, high_mixed, norm_train, norm_step,
):
    bf16, f32 = jnp.bfloat16, jnp.float32
    args = (
        train_query, low_query.T, high_query, train_key, low_key.T, high_key, train_value, low_value.T, high_value,
        train_mixed.T, low_mixed.T, high_mixed, norm_train.reshape(1, -1), norm_step.reshape(1, -1),
    )
    vmem = pltpu.MemorySpace.VMEM
    q_all, k_all, v_all, m_all, n_all = pl.pallas_call(
        gather_kernel,
        name="gather",
        out_shape=[
            vmem((5120, 1024), bf16), vmem((5120, 128), bf16), vmem((5120, 128), bf16),
            vmem((8, 1024, 640), bf16), vmem((8, 4, 4, 1, 128), f32),
        ],
        in_specs=[pl.BlockSpec(memory_space=pltpu.MemorySpace.HBM)] * 14,
        out_specs=[pl.BlockSpec(memory_space=vmem)] * 5,
        scratch_shapes=[pltpu.VMEM(a.shape, a.dtype) for a in args] + [
            pltpu.VMEM((320, 512), bf16), pltpu.VMEM((32, 320), bf16), pltpu.VMEM((4, 640, 128), f32),
            pltpu.SemaphoreType.DMA((N_LOADS,)), pltpu.SemaphoreType.DMA((8,)),
            pltpu.SemaphoreType.DMA((len(SLOTS),)), pltpu.SemaphoreType.DMA((4,)),
            pltpu.SemaphoreType.DMA((4,)), pltpu.SemaphoreType.DMA((18,)),
        ],
        compiler_params=pltpu.CompilerParams(
            collective_id=0, has_side_effects=True, vmem_limit_bytes=36 * 1024 * 1024
        ),
    )(*args)
    hbm = pltpu.MemorySpace.HBM
    q, k, v, m, n = pl.pallas_call(
        write_kernel,
        name="write",
        out_shape=[
            jax.ShapeDtypeStruct((5120, 1024), bf16), jax.ShapeDtypeStruct((5120, 128), bf16),
            jax.ShapeDtypeStruct((5120, 128), bf16), jax.ShapeDtypeStruct((1024, 5120), bf16),
            jax.ShapeDtypeStruct((40, 128), bf16),
        ],
        in_specs=[pl.BlockSpec(memory_space=vmem)] * 5,
        out_specs=[pl.BlockSpec(memory_space=hbm)] * 5,
        scratch_shapes=[pltpu.VMEM((40, 128), f32), pltpu.VMEM((40, 128), bf16), pltpu.SemaphoreType.DMA((13,))],
        compiler_params=pltpu.CompilerParams(vmem_limit_bytes=2 * 1024 * 1024),
    )(q_all, k_all, v_all, m_all, n_all)
    return q, k, v, m, n.reshape(5120)


def solution(mesh):
    return jax.shard_map(
        body,
        mesh=mesh,
        in_specs=(
            P("shard", "tp"), P("shard", None), P(None, "tp"),
            P("shard", "tp"), P("shard", None), P(None, "tp"),
            P("shard", "tp"), P("shard", None), P(None, "tp"),
            P("tp", "shard"), P("tp", None), P(None, "shard"),
            P(("shard", "tp")), P(("shard", "tp")),
        ),
        out_specs=(P(None, "tp"), P(None, "tp"), P(None, "tp"), P("tp", None), P()),
        check_vma=False,
    )
```

```python
import functools
import heapq

import jax
import jax.numpy as jnp
from jax import lax
from jax.experimental import pallas as pl
from jax.experimental.pallas import tpu as pltpu
from jax.sharding import PartitionSpec as P

MESH = pl.DeviceIdType.MESH
mix_rate = 0.5

Q_ROWS = 160
M_ROWS = 256
KIND = (0, 1, 0, 2, 3, 3, 0, 3, 3, 3)
FROM = (0, 0, 1, 0, 0, 1, 0, 0, 1, 1.75)
WEIGHT = (1, 1, 1, 1, 1, 1, 2, 2, 0.75, 0.25)
SIZES = (327680, 81920, 327680, 81920, 327680, 327680, 655360, 655360, 245760, 81920)
ONWARD = {"x+": {6: 0, 0: 0, 1: 1, 7: 4}, "x-": {6: 2, 2: 2, 3: 3, 7: 5}}
PARTNERS = {"x+": (0, 1, 2, 3), "x-": (2, 3, 0, 1)}


def own_sends(chunk, along_x, along_z):
    sends = []
    if along_z:
        sends.append(("z", ("z", 0, chunk)))
    if along_x:
        sends += [("x+", ("x+", 0, 3, chunk)), ("x-", ("x-", 0, 1, chunk))]
    if along_z:
        sends.append(("d", ("d", 0, 0, chunk)))
    return sends


def react(event):
    kind = event[0]
    if kind == "z":
        _, dx, chunk = event
        return [("d", ("d", 1, dx, chunk))]
    _, dz, dx, chunk = event
    sends = []
    if dx != 2 and chunk in ONWARD[kind]:
        sends.append((kind, (kind, dz, 2, ONWARD[kind][chunk])))
        if (dz, chunk) == (0, 7):
            sends += [(kind, (kind, 1, dx, other)) for other in PARTNERS[kind]]
    if KIND[chunk] == 3 and dz == 0:
        sends += [("z", ("z", dx, part)) for part in ((8, 9) if chunk == 5 else (chunk,))]
    sends.append(("d", ("d", dz, dx, chunk)))
    return sends


def plan():
    first = []
    for chunk in (6,):
        first += own_sends(chunk, True, True)
    second = []
    for chunk in (1, 3):
        second += own_sends(chunk, False, True)
    third = []
    for chunk in (7,):
        third += own_sends(chunk, True, True)
    for chunk in (1, 3):
        third += own_sends(chunk, True, False)
    starts = [(2.0, first), (2.2, second), (5.5, third)]
    heap, count, free, order = [], 0, {}, []
    for time, sends in starts:
        heapq.heappush(heap, (time, count, None, sends))
        count += 1
    while heap:
        time, _, event, sends = heapq.heappop(heap)
        if event is not None:
            order.append((time, event))
            sends = react(event)
        for link, item in sends:
            if link == "d":
                continue
            done = max(time, free.get(link, 0.0)) + SIZES[item[-1]] / 45000.0
            free[link] = done
            heapq.heappush(heap, (done + 1.9, count, item, None))
            count += 1
    order += [(t, (name,)) for t, name in ((30.0, "n1"), (42.0, "n2"), (45.0, "n3"), (48.0, "n4"), (51.0, "n5"), (60.0, "n6"))]
    order = [event for _, event in sorted(order, key=lambda pair: pair[0])]
    held = [order.index(("x+", 0, 3, 7)), order.index(("x-", 0, 1, 7))]
    assert min(held) > max(order.index(("z", 0, chunk)) for chunk in (6, 1, 3))
    return first, second, third, order


def slots():
    found = {}
    for event in plan()[3]:
        if event[0][0] != "n":
            dz, dx = (1, event[1]) if event[0] == "z" else (event[1], event[2])
            found[(dz, dx, event[-1])] = len(found)
    return found


SLOTS = slots()
N_LOADS = 14


def gather_kernel(
    tq, lq, hq, tk, lk, hk, tv, lv, hv, tm, lm, hm, n1, n2,
    q_all, k_all, v_all, m_all, n_all,
    tq_v, lq_v, hq_v, tk_v, lk_v, hk_v, tv_v, lv_v, hv_v, tm_v, lm_v, hm_v, n1_v, n2_v,
    tm_s, hm_s, turn,
    load_sem, send_sem, arrive_sem, sib_sem, pair_sem, norm_sem,
):
    sh = lax.axis_index("shard")
    tp = lax.axis_index("tp")
    core = lax.rem(sh, 2)
    x = lax.rem(sh // 2, 4)
    z = (sh // 8) * 2 + tp // 4
    y = lax.rem(tp, 4)

    def device(dx=0, dz=0, dy=0, other=False):
        zz = lax.rem(z + dz, 4)
        cc = 1 - core if other else core
        return (
            ((zz // 2) * 4 + lax.rem(x + dx, 4)) * 2 + cc,
            lax.rem(zz, 2) * 4 + lax.rem(y + dy, 4),
        )

    target = {
        "x+": device(dx=1), "x-": device(dx=3), "z": device(dz=2), "d": device(other=True),
    }

    loads = [
        pltpu.make_async_copy(src, dst, load_sem.at[k])
        for k, (src, dst) in enumerate((
            (lq, lq_v), (hq, hq_v), (tq, tq_v), (n1, n1_v), (n2, n2_v), (tm, tm_v), (hm, hm_v), (lm, lm_v),
            (tk, tk_v), (lk, lk_v), (hk, hk_v), (tv, tv_v), (lv, lv_v), (hv, hv_v),
        ))
    ]
    for copy in loads[:5]:
        copy.start()

    beside = device(dz=1 + 2 * lax.rem(z, 2))
    pair = device(dy=1 + 2 * lax.rem(y, 2))
    inner = lax.rem((y + 1) // 2, 2)
    across = device(dy=7 - 2 * y)
    partners = [target["z"]] + [device(dx=k) for k in (3, 1, 2)] + [beside, pair, target["d"]]
    barrier = pltpu.get_barrier_semaphore()
    for partner in partners:
        pl.semaphore_signal(barrier, inc=1, device_id=partner, device_id_type=MESH)

    @pl.when(inner == 1)
    def _():
        pl.semaphore_signal(barrier, inc=1, device_id=across, device_id_type=MESH)


    for copy in loads[5:]:
        copy.start()

    def send(src, dst, sent, sem, to):
        copy = pltpu.make_async_remote_copy(
            src_ref=src, dst_ref=dst, send_sem=sent, recv_sem=sem, device_id=to, device_id_type=MESH,
        )
        copy.start()
        return copy

    def waiting(ref, sent, sem):
        return pltpu.make_async_remote_copy(
            src_ref=ref, dst_ref=ref, send_sem=sent, recv_sem=sem, device_id=target["d"], device_id_type=MESH,
        )

    def arrived(dst, sem):
        waiting(dst, send_sem.at[0], sem).wait_recv()

    n_sent = [[0, 0] for _ in range(4)]

    def many(kind, count):
        if kind == 0:
            return q_all.at[pl.ds(0, Q_ROWS * count)]
        if kind < 3:
            return (k_all if kind == 1 else v_all).at[pl.ds(0, 320 * count)]
        if count % 4 == 0:
            return m_all.at[pl.ds(0, count // 4)]
        return m_all.at[pl.ds(0, count // 2), pl.ds(0, 512)]

    def place(chip, cc, chunk):
        row = (chip * 2 + cc) * 320
        if KIND[chunk] in (1, 2):
            return (k_all if KIND[chunk] == 1 else v_all).at[pl.ds(pl.multiple_of(row, 64), 320)]
        if KIND[chunk] == 0:
            return q_all.at[pl.ds(pl.multiple_of(row + Q_ROWS * FROM[chunk], 32), Q_ROWS * WEIGHT[chunk])]
        return m_all.at[
            chip, pl.ds(pl.multiple_of(512 * cc + int(M_ROWS * FROM[chunk]), 64), int(M_ROWS * WEIGHT[chunk]))
        ]

    def chip_at(dz2, dx):
        return (lax.rem(sh // 8 + dz2, 2)) * 4 + lax.rem(x + dx, 4)

    def arrive_index(dz, dx, chunk):
        return SLOTS[(dz, dx, chunk)]

    def dispatch(link, item, src, chip):
        kind, chunk = KIND[item[-1]], item[-1]
        if link == "d":
            sem, side = sib_sem.at[kind], 1
        else:
            dz, dx = (1, item[1]) if link == "z" else (item[1], item[2])
            sem, side = arrive_sem.at[arrive_index(dz, dx, chunk)], 0
        n_sent[kind][side] += WEIGHT[chunk]
        send(src, src, send_sem.at[kind * 2 + side], sem, target[link])

    first, second, third, order = plan()
    own = chip_at(0, 0)

    def wait_loads(*which):
        for k in which:
            loads[k].wait()

    def product(low_turned, high):
        return mix_rate * lax.dot_general(
            low_turned, high, (((0,), (0,)), ((), ())), preferred_element_type=jnp.float32
        )

    row = sh * 320
    wait_loads(3, 4)
    plane = core * 4 + y
    n_all[plane, z, x] = jnp.zeros((1, 128), jnp.float32)
    n_all[plane, z, x, :, 0:40] = n1_v[...] + n2_v[...]
    wait_loads(0, 1, 2)
    q_all[pl.ds(pl.multiple_of(row, 64), 320)] = (
        tq_v[...].astype(jnp.float32) + product(lq_v[...], hq_v[...])
    ).astype(jnp.bfloat16)
    pl.semaphore_wait(barrier, len(partners) + inner)
    line = n_all.at[plane, z, x]
    for k in (1, 2, 3):
        send(line, line, norm_sem.at[1], norm_sem.at[0], device(dx=k))
    three = n_all.at[plane, z, pl.ds(0, 3)]
    small = [waiting(three, norm_sem.at[1], norm_sem.at[0])]
    for link, item in first:
        dispatch(link, item, place(own, core, item[-1]), own)

    half = pl.ds(pl.multiple_of(512 * core, 512), 512)
    other_half = pl.ds(pl.multiple_of(512 * (1 - core), 512), 512)
    wait_loads(5, 6)
    small += [
        send(tm_v.at[:, other_half], tm_s, pair_sem.at[2], pair_sem.at[0], target["d"]),
        send(hm_v, hm_s, pair_sem.at[3], pair_sem.at[1], target["d"]),
    ]

    wait_loads(8, 9, 10, 11, 12, 13)
    k_all[pl.ds(pl.multiple_of(row, 64), 320)] = (
        tk_v[...].astype(jnp.float32) + product(lk_v[...], hk_v[...])
    ).astype(jnp.bfloat16)
    v_all[pl.ds(pl.multiple_of(row, 64), 320)] = (
        tv_v[...].astype(jnp.float32) + product(lv_v[...], hv_v[...])
    ).astype(jnp.bfloat16)
    for link, item in second:
        dispatch(link, item, place(own, core, item[-1]), own)

    wait_loads(7)
    arrived(tm_s, pair_sem.at[0])
    arrived(hm_s, pair_sem.at[1])
    mine = pl.ds(pl.multiple_of(320 * core, 64), 320)
    others = pl.ds(pl.multiple_of(320 * (1 - core), 64), 320)
    low_half = lm_v[:, half]
    own_half = tm_v[:, half]
    for b in range(4):
        cols = slice(128 * b, 128 * (b + 1))
        low = low_half[:, cols]
        turn[b, mine] = own_half[:, cols].astype(jnp.float32) + product(hm_v[...], low)
        turn[b, others] = tm_s[:, cols].astype(jnp.float32) + product(hm_s[...], low)
        rows = pl.ds(pl.multiple_of(512 * core + 128 * b, 128), 128)
        m_all[own, rows] = turn[b].T.astype(jnp.bfloat16)
    arrived(three, norm_sem.at[0])
    line = n_all.at[plane, z]
    small.append(send(line, line, norm_sem.at[8], norm_sem.at[2], beside))
    for link, item in third:
        dispatch(link, item, place(own, core, item[-1]), own)

    for event in order:
        kind, chunk = event[0], event[-1]
        if kind == "n1":
            arrived(n_all.at[plane, lax.rem(z + 1 + 2 * lax.rem(z, 2), 4)], norm_sem.at[2])
            line = n_all.at[plane, pl.ds((z // 2) * 2, 2)]
            small.append(send(line, line, norm_sem.at[9], norm_sem.at[3], target["z"]))
        elif kind == "n2":
            arrived(n_all.at[plane, pl.ds((1 - z // 2) * 2, 2)], norm_sem.at[3])
            line = n_all.at[plane]
            small.append(send(line, line, norm_sem.at[10], norm_sem.at[4], pair))
        elif kind == "n3":
            arrived(n_all.at[core * 4 + y + 1 - 2 * lax.rem(y, 2)], norm_sem.at[4])
            near = n_all.at[pl.ds(core * 4 + (y // 2) * 2, 2)]
            far = n_all.at[pl.ds(core * 4 + (1 - y // 2) * 2, 2)]

            @pl.when(inner == 1)
            def _():
                send(near, near, norm_sem.at[11], norm_sem.at[5], across)
        elif kind == "n4":

            @pl.when(inner == 1)
            def _():
                arrived(far, norm_sem.at[5])
                send(far, far, norm_sem.at[12], norm_sem.at[6], pair)
        elif kind == "n5":

            @pl.when(inner == 0)
            def _():
                arrived(far, norm_sem.at[6])

            line = n_all.at[pl.ds(core * 4, 4)]
            small.append(send(line, line, norm_sem.at[13], norm_sem.at[7], target["d"]))
        elif kind == "n6":
            arrived(n_all.at[pl.ds((1 - core) * 4, 4)], norm_sem.at[7])

            @pl.when(inner == 1)
            def _():
                waiting(near, norm_sem.at[11], norm_sem.at[5]).wait_send()
                waiting(far, norm_sem.at[12], norm_sem.at[6]).wait_send()

            for copy in small:
                copy.wait_send()
        else:
            dz, dx = (1, event[1]) if kind == "z" else (event[1], event[2])
            chip = chip_at(dz, dx)
            src = place(chip, core, chunk)
            arrived(src, arrive_sem.at[arrive_index(dz, dx, chunk)])
            for link, item in react(event):
                at = chip_at(1, 0) if dz == 0 and item[0] == kind and item[1] == 1 else chip
                dispatch(link, item, place(at, core, item[-1]), at)

    for kind, per_piece in enumerate((2, 1, 1, 2)):
        for side in (0, 1):
            count = int(n_sent[kind][side])
            waiting(many(kind, count), send_sem.at[kind * 2 + side], sib_sem.at[0]).wait_send()
        arrived(many(kind, per_piece * 8), sib_sem.at[kind])


def write_kernel(q_all, k_all, v_all, m_all, n_all, q_out, k_out, v_out, m_out, n_out, lines, rounded, sems):
    copies = []
    for k in range(8):
        copies.append((m_all.at[k], m_out.at[:, pl.ds(640 * k, 640)]))
        if k % 4 == 0:
            copies.append((q_all.at[pl.ds(640 * k, 2560)], q_out.at[pl.ds(640 * k, 2560)]))
    copies += [(k_all, k_out), (v_all, v_out)]
    copies = [pltpu.make_async_copy(src, dst, sems.at[k]) for k, (src, dst) in enumerate(copies)]
    for copy in copies:
        copy.start()
    lane = lax.broadcasted_iota(jnp.int32, (8, 128), 1)
    acc = [jnp.zeros((8, 128), jnp.float32) for _ in range(5)]
    for i in range(16):
        core, zl, y = i // 8, (i // 4) % 2, i % 4
        rows = [n_all[core * 4 + y, zh * 2 + zl, xx] for zh in range(2) for xx in range(4)]
        block = jnp.concatenate(rows, axis=0)
        q, off = (40 * i) // 128, (40 * i) % 128
        turned = pltpu.roll(block, off, 1) if off else block
        acc[q] = jnp.where((lane >= off) & (lane < off + 40), turned, acc[q])
        if off + 40 > 128:
            acc[q + 1] = jnp.where(lane < off + 40 - 128, turned, acc[q + 1])
    for q in range(5):
        lines[pl.ds(q, 8, stride=5), :] = acc[q]
    rounded[...] = lines[...].astype(jnp.bfloat16)
    last = pltpu.make_async_copy(rounded, n_out, sems.at[len(copies)])
    last.start()
    copies.append(last)
    for copy in copies:
        copy.wait()


def body(
    train_query, low_query, high_query, train_key, low_key, high_key, train_value, low_value, high_value,
    train_mixed, low_mixed, high_mixed, norm_train, norm_step,
):
    bf16, f32 = jnp.bfloat16, jnp.float32
    args = (
        train_query, low_query.T, high_query, train_key, low_key.T, high_key, train_value, low_value.T, high_value,
        train_mixed.T, low_mixed.T, high_mixed, norm_train.reshape(1, -1), norm_step.reshape(1, -1),
    )
    vmem = pltpu.MemorySpace.VMEM
    q_all, k_all, v_all, m_all, n_all = pl.pallas_call(
        gather_kernel,
        name="gather",
        out_shape=[
            vmem((5120, 1024), bf16), vmem((5120, 128), bf16), vmem((5120, 128), bf16),
            vmem((8, 1024, 640), bf16), vmem((8, 4, 4, 1, 128), f32),
        ],
        in_specs=[pl.BlockSpec(memory_space=pltpu.MemorySpace.HBM)] * 14,
        out_specs=[pl.BlockSpec(memory_space=vmem)] * 5,
        scratch_shapes=[pltpu.VMEM(a.shape, a.dtype) for a in args] + [
            pltpu.VMEM((320, 512), bf16), pltpu.VMEM((32, 320), bf16), pltpu.VMEM((4, 640, 128), f32),
            pltpu.SemaphoreType.DMA((N_LOADS,)), pltpu.SemaphoreType.DMA((8,)),
            pltpu.SemaphoreType.DMA((len(SLOTS),)), pltpu.SemaphoreType.DMA((4,)),
            pltpu.SemaphoreType.DMA((4,)), pltpu.SemaphoreType.DMA((14,)),
        ],
        compiler_params=pltpu.CompilerParams(
            collective_id=0, has_side_effects=True, vmem_limit_bytes=36 * 1024 * 1024
        ),
    )(*args)
    hbm = pltpu.MemorySpace.HBM
    q, k, v, m, n = pl.pallas_call(
        write_kernel,
        name="write",
        out_shape=[
            jax.ShapeDtypeStruct((5120, 1024), bf16), jax.ShapeDtypeStruct((5120, 128), bf16),
            jax.ShapeDtypeStruct((5120, 128), bf16), jax.ShapeDtypeStruct((1024, 5120), bf16),
            jax.ShapeDtypeStruct((40, 128), bf16),
        ],
        in_specs=[pl.BlockSpec(memory_space=vmem)] * 5,
        out_specs=[pl.BlockSpec(memory_space=hbm)] * 5,
        scratch_shapes=[pltpu.VMEM((40, 128), f32), pltpu.VMEM((40, 128), bf16), pltpu.SemaphoreType.DMA((13,))],
        compiler_params=pltpu.CompilerParams(vmem_limit_bytes=2 * 1024 * 1024),
    )(q_all, k_all, v_all, m_all, n_all)
    return q, k, v, m, n.reshape(5120)


def solution(mesh):
    return jax.shard_map(
        body,
        mesh=mesh,
        in_specs=(
            P("shard", "tp"), P("shard", None), P(None, "tp"),
            P("shard", "tp"), P("shard", None), P(None, "tp"),
            P("shard", "tp"), P("shard", None), P(None, "tp"),
            P("tp", "shard"), P("tp", None), P(None, "shard"),
            P(("shard", "tp")), P(("shard", "tp")),
        ),
        out_specs=(P(None, "tp"), P(None, "tp"), P(None, "tp"), P("tp", None), P()),
        check_vma=False,
    )
```
